32 devices in a mesh: section: 2 (over core), rows: 16 (over z, y, x).
Axes of the slice: x: 2, y: 2, z: 4, core: 2. Of those that a mesh axis runs over, the one named last changes fastest.
Arguments:
- table: float32 [16384, 64], P('rows', 'section'), may hold values from -6 to 6
- mask: int32 [16384], P('rows'), may hold values from 0 to 1, as said below
- weight: float32 [64, 1024], replicated, may hold values from -0.75 to 0.75
- bias: float32 [1024], replicated, may hold values from -3 to 3
Outputs:
- projected: bfloat16 [16384, 1024], P('rows', 'section')
The draws below stay inside these ranges and needn't reach their ends.
Inputs may be any that keep to these rules, and one draw needn't show every extreme that they name: `mask`: the probability that a row survives is constant within one device's rows and drawn afresh for each device, from about 5 to 95 percent.
All inputs are finite; a program needn't handle non-finite values.
Results may differ from the reference program's by a relative error of at most 0.001.
Values sent between devices are 32-bit elements; how exact they have to be, the bound alone decides.
A program may use at most 64 MiB of HBM per device.

```python
import jax
import jax.numpy as jnp
from jax import lax

C = 64
F = 1024
ROWS_DEV = 1024
TOTAL = 16384
N_ROWS = 16


def draw_mask(key, part):
    blocks = TOTAL // ROWS_DEV
    first, second = jax.random.split(jax.random.fold_in(key, 11))
    rates = jax.random.randint(first, (blocks,), 50, 950)
    levels = jnp.repeat(rates, ROWS_DEV)
    ticket = jax.random.randint(second, (TOTAL,), 0, 1000)
    return (ticket < levels).astype(jnp.int32)


def block_levels(key, extent, cuts, smallest, largest):
    factor_of, own = 1.0, jax.random.fold_in(key, 6)
    for axis_at, parts in cuts:
        draws = jnp.exp(jax.random.uniform(jax.random.fold_in(own, axis_at), (parts,), jnp.float32, smallest / len(cuts), largest / len(cuts)))
        factor_of = factor_of * jnp.repeat(draws, extent[axis_at] // parts).reshape([-1 if axis == axis_at else 1 for axis in range(len(extent))])
    return factor_of


def noise(rng, dims, scale, limit, shards=(), kind=jnp.bfloat16):
    gain = block_levels(rng, dims, shards, -0.22, 0.18) if shards else 1.0
    array = jax.random.normal(rng, dims, jnp.float32) * scale * gain
    return jnp.minimum(jnp.maximum(array, -limit), limit).astype(kind)


def setup_inputs(seed: int = 0) -> dict:
    key_of = jax.random.split(jax.random.key(seed), 5)
    table = noise(key_of[0], (TOTAL, C), 1.0, 6.0, ((0, 16), (1, 2)), jnp.float32)
    mask = draw_mask(jax.random.fold_in(key_of[4], 71), 0)
    weight = noise(key_of[2], (C, F), C ** -0.5, 0.75, (), jnp.float32)
    bias = noise(key_of[3], (F,), 0.5, 3.0, (), jnp.float32)
    return dict(table=table, mask=mask, weight=weight, bias=bias)


def reference(table, mask, weight, bias):
    rank = (jnp.cumsum(mask) - mask).astype(jnp.int32)
    total = jnp.sum(mask).astype(jnp.int32)
    place = jnp.where(mask == 1, rank, TOTAL).astype(jnp.int32)
    packed = jnp.zeros((TOTAL, C), jnp.float32).at[place].set(table, mode="drop")
    blocks = packed.reshape(N_ROWS, ROWS_DEV, C)
    starts = jnp.arange(N_ROWS, dtype=jnp.int32)

    def project(args):
        block, start = args
        result = jnp.dot(block, weight, precision=lax.Precision.HIGHEST, preferred_element_type=jnp.float32) + bias
        filled = start * ROWS_DEV + jnp.arange(ROWS_DEV, dtype=jnp.int32) < total
        return jnp.where(filled[:, None], result, 0.0).astype(jnp.bfloat16)

    projected = lax.map(project, (blocks, starts))
    return projected.reshape(TOTAL, F)
```

```python
import functools

import jax
import jax.numpy as jnp
from jax import lax
from jax.experimental import pallas as pl
from jax.experimental.pallas import tpu as pltpu
from jax.sharding import PartitionSpec as P

CHUNKS = 4
PLANE = 4
RAW = 4
LINES = 4
GROUP = 8
TERMS = 2
F32 = jnp.float32
BF16 = jnp.bfloat16
I32 = jnp.int32


def split(x, terms):
    parts = []
    for _ in range(terms):
        part = x.astype(BF16)
        parts.append(part)
        x = x - part.astype(F32)
    return parts


def butterfly(
    n, table_hbm, mask_hbm, w_hbm, bias_hbm, out_ref,
    table_ref, mask_ref, bias_ref,
    tally, planes, prefix, raw, hold, came, joined, w_ref, wcat,
    send_sem, recv_sem, raw_send, raw_recv, count_send, count_recv, plane_send, plane_recv, load_sem,
):
    half, height = table_hbm.shape
    width = out_ref.shape[1]
    lines = height // 128
    levels = (n - 1).bit_length()
    lanes = height // CHUNKS
    side = min(PLANE, n)
    crowd = min(RAW, n)
    first = (crowd - 1).bit_length()
    count_planes = n // side
    me = lax.axis_index("rows")
    core = lax.axis_index("section")
    plane = me // side
    seat = lax.rem(me, side)

    columns = pl.ds(pl.multiple_of(core * width, 128), width)
    mask_copy = pltpu.make_async_copy(mask_hbm, mask_ref, load_sem.at[0])
    table_copy = pltpu.make_async_copy(table_hbm, table_ref, load_sem.at[1])
    w_copy = pltpu.make_async_copy(w_hbm.at[:, columns], w_ref, load_sem.at[2])
    bias_copy = pltpu.make_async_copy(bias_hbm.at[:, columns], bias_ref, load_sem.at[3])
    for load in (mask_copy, table_copy, w_copy, bias_copy):
        load.start()

    def seat_peer(step):
        return plane * side + lax.rem(seat + step, side)

    def plane_peer(step):
        return lax.rem(plane + step, count_planes) * side + seat

    barrier = pltpu.get_barrier_semaphore()
    for step in range(1, side):
        pl.semaphore_signal(barrier, inc=1, device_id={"rows": seat_peer(step)})
    for step in range(1, count_planes):
        pl.semaphore_signal(barrier, inc=1, device_id={"rows": plane_peer(step)})
    pl.semaphore_signal(barrier, inc=1, device_id={"section": 1 - core})

    mask_copy.wait()
    mask = mask_ref[...]
    ones = mask.astype(F32).astype(BF16)
    row = lax.broadcasted_iota(I32, (128, 128), 0)
    col = lax.broadcasted_iota(I32, (128, 128), 1)
    before = jnp.where(row < col, 1.0, 0.0).astype(BF16)
    inner = jnp.dot(ones, before, preferred_element_type=F32).astype(I32)
    sums = jnp.dot(ones, jnp.ones((128, 128), BF16), preferred_element_type=F32).astype(I32)
    running = jnp.zeros((1, 128), I32)
    starts = []
    for line in range(lines):
        starts.append(running)
        running = running + sums[line : line + 1]
    tally[seat] = running
    slot = jnp.where(mask == 1, inner + jnp.concatenate(starts, 0), -1)

    own = lax.rem(me, crowd)
    table_copy.wait()
    turned = jnp.concatenate(split(table_ref[...], 3), 0)
    for chunk in range(CHUNKS):
        here = chunk * lanes + lax.broadcasted_iota(I32, (lanes, 128), 0)
        hot = jnp.concatenate(
            [jnp.where(here == slot[b : b + 1], 1.0, 0.0).astype(BF16) for b in range(chunk * lanes // 128, lines)], 1
        )
        folded = lax.dot_general(
            turned[:, chunk * lanes :], hot, (((1,), (1,)), ((), ())), preferred_element_type=F32
        )
        raw[own, :, chunk * lanes : (chunk + 1) * lanes] = (
            folded[:half] + folded[half : 2 * half]
        ) + folded[2 * half :]

    pl.semaphore_wait(barrier, side + count_planes - 1)

    def seat_copy(step):
        return pltpu.make_async_remote_copy(
            src_ref=tally.at[seat], dst_ref=tally.at[seat],
            send_sem=count_send.at[step], recv_sem=count_recv.at[step],
            device_id={"rows": seat_peer(step)},
        )

    def plane_copy(step):
        return pltpu.make_async_remote_copy(
            src_ref=planes.at[plane], dst_ref=planes.at[plane],
            send_sem=plane_send.at[step], recv_sem=plane_recv.at[step],
            device_id={"rows": plane_peer(step)},
        )

    def raw_copy(step):
        return pltpu.make_async_remote_copy(
            src_ref=raw.at[own], dst_ref=raw.at[own],
            send_sem=raw_send.at[step], recv_sem=raw_recv.at[step],
            device_id={"rows": me - own + lax.rem(own + step, crowd)},
        )

    for step in range(1, side):
        seat_copy(step).start()
    for step in range(1, crowd):
        raw_copy(step).start()
    for step in range(1, side):
        seat_copy(step).wait_recv()
    everyone = jnp.zeros((1, 128), I32)
    for at in range(side):
        everyone = everyone + tally[at]
    planes[plane] = everyone
    for step in range(1, count_planes):
        plane_copy(step).start()

    w_copy.wait()
    bias_copy.wait()
    bias = bias_ref[...]
    w_hi, w_lo = split(w_ref[...], 2)
    b_hi, b_mid, b_lo = [part.astype(F32) for part in split(bias, 3)]
    line = lax.broadcasted_iota(I32, (16, width), 0)
    extra = jnp.where(line == 0, b_hi, jnp.where(line == 1, b_mid, jnp.where(line == 2, b_lo, 0.0)))
    wcat[...] = jnp.concatenate([w_hi, w_lo, w_hi, extra.astype(BF16)], 0)

    for step in range(1, count_planes):
        plane_copy(step).wait_recv()
    total = jnp.zeros((1, 128), I32)
    for at in range(count_planes):
        prefix[at * side] = total
        total = total + planes[at]
    prefix[n] = total
    running = prefix[plane * side]
    for at in range(side - 1):
        running = running + tally[at]
        prefix[plane * side + at + 1] = running

    def wide(x):
        return jnp.concatenate([x] * (lanes // 128), 1)

    def data_copy(level, chunk):
        at = (slice(None), pl.ds(chunk * lanes, lanes))
        return pltpu.make_async_remote_copy(
            src_ref=hold.at[(level,) + at], dst_ref=came.at[(level,) + at],
            send_sem=send_sem.at[level, chunk], recv_sem=recv_sem.at[level, chunk],
            device_id={"rows": me + (1 - 2 * (me // (1 << level) % 2)) * (1 << level)},
        )

    def join_copy(chunk):
        at = (core, slice(None), pl.ds(chunk * lanes, lanes))
        return pltpu.make_async_remote_copy(
            src_ref=joined.at[at], dst_ref=joined.at[at],
            send_sem=send_sem.at[levels, chunk], recv_sem=recv_sem.at[levels, chunk],
            device_id={"section": 1 - core},
        )

    for step in range(1, crowd):
        raw_copy(step).wait_recv()
    turns = []
    for at in range(crowd):
        shift = (prefix[me - own + at] & (height - 1))[0, 0]
        turns.append(pltpu.roll(raw[at], shift, 1))
    low = wide(prefix[me - own])
    for chunk in range(CHUNKS):
        at = slice(chunk * lanes, (chunk + 1) * lanes)
        base = own * height + chunk * lanes + lax.broadcasted_iota(I32, (1, lanes), 1)
        place = low + ((base - low) & (crowd * height - 1))
        place = jnp.broadcast_to(place, (half, lanes))
        block = turns[0][:, at]
        for other in range(1, crowd):
            block = jnp.where(place >= wide(prefix[me - own + other]), turns[other][:, at], block)
        hold[first, :, at] = block
        data_copy(first, chunk).start()

    for level in range(first, levels):
        reach = 2 << level
        group = me // reach * reach
        bit = me // (1 << level) % 2
        low = wide(prefix[group])
        middle = wide(prefix[group + (1 << level)])
        for chunk in range(CHUNKS):
            at = slice(chunk * lanes, (chunk + 1) * lanes)
            data_copy(level, chunk).wait_recv()
            base = (me % reach) * height + chunk * lanes
            base = base + lax.broadcasted_iota(I32, (1, lanes), 1)
            place = low + ((base - low) & (reach * height - 1))
            upper = jnp.where(place >= middle, 1, 0)
            foreign = jnp.broadcast_to(upper, (half, lanes)) != bit
            block = jnp.where(foreign, came[level, :, at], hold[level, :, at])
            if level < levels - 1:
                hold[level + 1, :, at] = block
                data_copy(level + 1, chunk).start()
            else:
                joined[core, :, at] = block
                join_copy(chunk).start()

    ends = wide(total)
    for chunk in range(CHUNKS):
        at = slice(chunk * lanes, (chunk + 1) * lanes)
        join_copy(chunk).wait_recv()
        owned = me * height + chunk * lanes + lax.broadcasted_iota(I32, (1, lanes), 1)
        filled = jnp.where(owned < ends, 1.0, 0.0)
        rows = jnp.concatenate([joined[0, :, at], joined[1, :, at]], 0)
        rows = jnp.where(jnp.broadcast_to(filled, rows.shape) > 0.5, rows, 0.0)
        a_hi, a_lo = split(rows, 2)
        marks = jnp.broadcast_to(filled, (16, lanes)).astype(BF16)
        lhs = jnp.concatenate([a_hi, a_hi, a_lo, marks], 0)
        out_ref[at, :] = lax.dot_general(
            lhs, wcat[...], (((0,), (0,)), ((), ())), preferred_element_type=F32
        ).astype(BF16)

    for step in range(1, side):
        seat_copy(step).wait_send()
    for step in range(1, count_planes):
        plane_copy(step).wait_send()
    for step in range(1, crowd):
        raw_copy(step).wait_send()
    for level in range(first, levels):
        for chunk in range(CHUNKS):
            data_copy(level, chunk).wait_send()
    for chunk in range(CHUNKS):
        join_copy(chunk).wait_send()


def wide(x, lanes):
    return jnp.concatenate([x] * (lanes // 128), 1)


def flip(at, step, extent):
    out, bit = 0, 1
    while bit < extent:
        a, b = at // bit % 2, step // bit % 2
        out = out + bit * (a + b - 2 * a * b)
        bit *= 2
    return out


def direct(
    n, table_hbm, mask_hbm, w_hbm, bias_hbm, out_ref,
    table_ref, mask_ref, bias_ref,
    tally, prefix, gather, turned, pieces, got, joined, w_ref, wcat,
    load_sem, count_send, count_recv, gather_send, gather_recv, relay_send,
    piece_send, piece_recv, join_send, join_recv,
):
    half, height = table_hbm.shape
    width = out_ref.shape[1]
    rows = height // 128
    lanes = height // CHUNKS
    groups = half // GROUP
    side = min(PLANE, n)
    lines = n // side
    me = lax.axis_index("rows")
    core = lax.axis_index("section")
    line = me // side
    seat = lax.rem(me, side)
    flat = core == 1

    columns = pl.ds(pl.multiple_of(core * width, 128), width)
    mask_copy = pltpu.make_async_copy(mask_hbm, mask_ref, load_sem.at[0])
    table_copy = pltpu.make_async_copy(table_hbm, table_ref, load_sem.at[1])
    w_copy = pltpu.make_async_copy(w_hbm.at[:, columns], w_ref, load_sem.at[2])
    bias_copy = pltpu.make_async_copy(bias_hbm.at[:, columns], bias_ref, load_sem.at[3])
    for load in (mask_copy, table_copy, w_copy, bias_copy):
        load.start()

    barrier = pltpu.get_barrier_semaphore()
    for step in range(1, n):
        pl.semaphore_signal(barrier, inc=1, device_id={"rows": lax.rem(me + step, n)})
    pl.semaphore_signal(barrier, inc=1, device_id={"section": 1 - core})

    mask_copy.wait()
    mask = mask_ref[...]
    ones = mask.astype(F32).astype(BF16)
    row = lax.broadcasted_iota(I32, (128, 128), 0)
    col = lax.broadcasted_iota(I32, (128, 128), 1)
    before = jnp.where(row < col, 1.0, 0.0).astype(BF16)
    inner = jnp.dot(ones, before, preferred_element_type=F32).astype(I32)
    sums = jnp.dot(ones, jnp.ones((128, 128), BF16), preferred_element_type=F32).astype(I32)
    running = jnp.zeros((1, 128), I32)
    starts = []
    for at in range(rows):
        starts.append(running)
        running = running + sums[at : at + 1]
    tally[me] = running
    slot = jnp.where(mask == 1, inner + jnp.concatenate(starts, 0), -1)

    own = jnp.where(flat, seat, line)
    table_copy.wait()
    terms = jnp.concatenate(split(table_ref[...], TERMS), 0)
    for chunk in range(CHUNKS):
        here = chunk * lanes + lax.broadcasted_iota(I32, (lanes, 128), 0)
        hot = jnp.concatenate(
            [jnp.where(here == slot[b : b + 1], 1.0, 0.0).astype(BF16) for b in range(chunk * lanes // 128, rows)], 1
        )
        folded = lax.dot_general(
            terms[:, chunk * lanes :], hot, (((1,), (1,)), ((), ())), preferred_element_type=F32
        )
        total = folded[:half]
        for term in range(1, TERMS):
            total = total + folded[term * half : (term + 1) * half]
        gather[own, :, chunk * lanes : (chunk + 1) * lanes] = total

    pl.semaphore_wait(barrier, n)

    def count_copy(step):
        return pltpu.make_async_remote_copy(
            src_ref=tally.at[me], dst_ref=tally.at[me],
            send_sem=count_send.at[step], recv_sem=count_recv.at[step],
            device_id={"rows": lax.rem(me + step, n)},
        )

    def seat_copy(step, g):
        at = (seat, pl.ds(g * GROUP, GROUP))
        return pltpu.make_async_remote_copy(
            src_ref=gather.at[at], dst_ref=gather.at[at],
            send_sem=gather_send.at[step, g], recv_sem=gather_recv.at[step, g],
            device_id={"rows": line * side + flip(seat, step, side)},
        )

    def line_copy(source, target, g):
        at = (source, pl.ds(g * GROUP, GROUP))
        return pltpu.make_async_remote_copy(
            src_ref=gather.at[at], dst_ref=gather.at[at],
            send_sem=gather_send.at[target, g], recv_sem=gather_recv.at[source, g],
            device_id={"rows": target * side + seat},
        )

    def relay_copy(source, g):
        at = (source, pl.ds(g * GROUP, GROUP))
        return pltpu.make_async_remote_copy(
            src_ref=gather.at[at], dst_ref=gather.at[at],
            send_sem=relay_send.at[source, g], recv_sem=gather_recv.at[source, g],
            device_id={"rows": side + seat},
        )

    def down_copy(source, target, g):
        at = pl.ds(g * GROUP, GROUP)
        return pltpu.make_async_remote_copy(
            src_ref=pieces.at[target, at], dst_ref=got.at[source, at],
            send_sem=piece_send.at[target, g], recv_sem=piece_recv.at[source, g],
            device_id={"rows": target * side + seat},
        )

    def across_copy(step, g):
        at = pl.ds(g * GROUP, GROUP)
        return pltpu.make_async_remote_copy(
            src_ref=pieces.at[step, at], dst_ref=got.at[step, at],
            send_sem=piece_send.at[step, g], recv_sem=piece_recv.at[step, g],
            device_id={"rows": line * side + flip(seat, step, side)},
        )

    def join_copy(g):
        at = (core, pl.ds(g * GROUP, GROUP))
        return pltpu.make_async_remote_copy(
            src_ref=joined.at[at], dst_ref=joined.at[at],
            send_sem=join_send.at[g], recv_sem=join_recv.at[g],
            device_id={"section": 1 - core},
        )

    for step in range(1, n):
        count_copy(step).start()

    @pl.when(flat)
    def _():
        for g in range(groups):
            for step in range(1, side):
                seat_copy(step, g).start()

    for source in range(1, lines):
        @pl.when(jnp.logical_and(core == 0, line == source))
        def _(source=source):
            for target in range(source):
                if target != 1:
                    for g in range(groups):
                        line_copy(source, target, g).start()

    w_copy.wait()
    bias_copy.wait()
    bias = bias_ref[...]
    w_hi, w_lo = split(w_ref[...], 2)
    b_hi, b_mid, b_lo = [part.astype(F32) for part in split(bias, 3)]
    at = lax.broadcasted_iota(I32, (16, width), 0)
    extra = jnp.where(at == 0, b_hi, jnp.where(at == 1, b_mid, jnp.where(at == 2, b_lo, 0.0)))
    wcat[...] = jnp.concatenate([w_hi, w_lo, w_hi, extra.astype(BF16)], 0)

    for step in range(1, n):
        count_copy(step).wait_recv()
    total = jnp.zeros((1, 128), I32)
    for at in range(n):
        prefix[at] = total
        total = total + tally[at]
    prefix[n] = total

    lane = lax.broadcasted_iota(I32, (GROUP, height), 1)

    def bound(index):
        return wide(jnp.broadcast_to(prefix[index], (GROUP, 128)), height)

    def turn(slot, index, g):
        shift = (prefix[index] & (height - 1))[0, 0]
        return pltpu.roll(gather[slot, g * GROUP : (g + 1) * GROUP], shift, 1)

    @pl.when(flat)
    def _():
        for g in range(groups):
            rows_g = slice(g * GROUP, (g + 1) * GROUP)
            for step in range(1, side):
                seat_copy(step, g).wait_recv()
            blocks = [turn(at, line * side + at, g) for at in range(side)]
            for target in range(lines):
                place = (target * side + seat) * height + lane
                piece = jnp.where(place >= bound(line * side), blocks[0], 0.0)
                for at in range(1, side):
                    piece = jnp.where(place >= bound(line * side + at), blocks[at], piece)
                pieces[target, rows_g] = jnp.where(place >= bound(line * side + side), 0.0, piece)
                if target == 0:
                    @pl.when(line > 0)
                    def _(g=g):
                        for source in range(1, lines):
                            @pl.when(line == source)
                            def _(source=source):
                                down_copy(source, 0, g).start()
        for source in range(2, lines):
            @pl.when(line == source)
            def _(source=source):
                for target in range(1, source):
                    for g in range(groups):
                        down_copy(source, target, g).start()

        for g in range(groups):
            rows_g = slice(g * GROUP, (g + 1) * GROUP)
            joined[1, rows_g] = pieces[line, rows_g]
            for source in range(1, lines):
                @pl.when(line < source)
                def _(source=source, g=g, rows_g=rows_g):
                    down_copy(source, line, g).wait_recv()
                    joined[1, rows_g] = joined[1, rows_g] + got[source, rows_g]
            join_copy(g).start()

    @pl.when(core == 0)
    def _():
        for g in range(groups):
            rows_g = slice(g * GROUP, (g + 1) * GROUP)
            for source in range(1, lines):
                @pl.when(line < source)
                def _(source=source, g=g):
                    line_copy(source, line, g).wait_recv()
                if source >= 2:
                    @pl.when(line == 0)
                    def _(source=source, g=g):
                        relay_copy(source, g).start()
            blocks = [turn(at, at * side + seat, g) for at in range(lines)]
            for step in list(range(1, side)) + [0]:
                place = (line * side + flip(seat, step, side)) * height + lane
                piece = jnp.zeros((GROUP, height), F32)
                for at in range(lines):
                    index = at * side + seat
                    inside = jnp.logical_and(place >= bound(index), place < bound(index + 1))
                    piece = jnp.where(inside, blocks[at], piece)
                pieces[step, rows_g] = piece
                if step:
                    across_copy(step, g).start()
        for g in range(groups):
            rows_g = slice(g * GROUP, (g + 1) * GROUP)
            total = pieces[0, rows_g]
            for step in range(1, side):
                across_copy(step, g).wait_recv()
                total = total + got[step, rows_g]
            joined[0, rows_g] = total
            join_copy(g).start()

    for g in range(groups):
        join_copy(g).wait_recv()
    ends = wide(prefix[n], lanes)
    for chunk in range(CHUNKS):
        at = slice(chunk * lanes, (chunk + 1) * lanes)
        owned = me * height + chunk * lanes + lax.broadcasted_iota(I32, (1, lanes), 1)
        filled = jnp.where(owned < ends, 1.0, 0.0)
        block = jnp.concatenate([joined[0, :, at], joined[1, :, at]], 0)
        a_hi, a_lo = split(block, 2)
        marks = jnp.broadcast_to(filled, (16, lanes)).astype(BF16)
        lhs = jnp.concatenate([a_hi, a_hi, a_lo, marks], 0)
        out_ref[at, :] = lax.dot_general(
            lhs, wcat[...], (((0,), (0,)), ((), ())), preferred_element_type=F32
        ).astype(BF16)

    for step in range(1, n):
        count_copy(step).wait_send()
    for g in range(groups):
        join_copy(g).wait_send()

    @pl.when(flat)
    def _():
        for g in range(groups):
            for step in range(1, side):
                seat_copy(step, g).wait_send()
        for source in range(1, lines):
            @pl.when(line == source)
            def _(source=source):
                for target in range(source):
                    for g in range(groups):
                        down_copy(source, target, g).wait_send()

    @pl.when(core == 0)
    def _():
        for source in range(1, lines):
            @pl.when(line == source)
            def _(source=source):
                for target in range(source):
                    if target != 1:
                        for g in range(groups):
                            line_copy(source, target, g).wait_send()
        for g in range(groups):
            for source in range(2, lines):
                @pl.when(line == 0)
                def _(source=source, g=g):
                    relay_copy(source, g).wait_send()
            for step in range(1, side):
                across_copy(step, g).wait_send()


def solution(mesh):
    n, sections = mesh.shape["rows"], mesh.shape["section"]

    def step(table, mask, weight, bias):
        height, half = table.shape
        cols, features = weight.shape
        width = features // sections
        levels = (n - 1).bit_length()
        side, crowd = min(PLANE, n), min(RAW, n)
        lines, groups = n // side, half // GROUP
        operands = table.T, mask.reshape(height // 128, 128), weight, bias.reshape(1, features)
        sem = pltpu.SemaphoreType.DMA
        loads = [
            pltpu.VMEM((half, height), F32),
            pltpu.VMEM((height // 128, 128), I32),
            pltpu.VMEM((1, width), F32),
        ]
        weights = [
            pltpu.VMEM((cols, width), F32),
            pltpu.VMEM((3 * cols + 16, width), BF16),
        ]
        if lines <= LINES:
            most = max(side, lines)
            block = pltpu.VMEM((most, half, height), F32)
            body = direct
            scratch = loads + [
                pltpu.VMEM((n, 1, 128), I32),
                pltpu.VMEM((n + 1, 1, 128), I32),
                block, block, block, block,
                pltpu.VMEM((sections, half, height), F32),
            ] + weights + [
                sem((4,)),
                sem((n,)), sem((n,)),
                sem((most, groups)), sem((most, groups)), sem((most, groups)),
                sem((most, groups)), sem((most, groups)),
                sem((groups,)), sem((groups,)),
            ]
        else:
            body = butterfly
            scratch = loads + [
                pltpu.VMEM((side, 1, 128), I32),
                pltpu.VMEM((n // side, 1, 128), I32),
                pltpu.VMEM((n + 1, 1, 128), I32),
                pltpu.VMEM((crowd, half, height), F32),
                pltpu.VMEM((levels, half, height), F32),
                pltpu.VMEM((levels, half, height), F32),
                pltpu.VMEM((sections, half, height), F32),
            ] + weights + [
                sem((levels + 1, CHUNKS)), sem((levels + 1, CHUNKS)),
                sem((crowd,)), sem((crowd,)),
                sem((side,)), sem((side,)),
                sem((n // side,)), sem((n // side,)),
                sem((4,)),
            ]
        return pl.pallas_call(
            functools.partial(body, n),
            name="filter_project",
            out_shape=jax.ShapeDtypeStruct((height, width), BF16),
            in_specs=[pl.BlockSpec(memory_space=pltpu.HBM)] * 4,
            out_specs=pl.BlockSpec(memory_space=pltpu.VMEM),
            scratch_shapes=scratch,
            compiler_params=pltpu.CompilerParams(
                collective_id=0, has_side_effects=True, vmem_limit_bytes=16 << 20
            ),
        )(*[pltpu.with_memory_space_constraint(x, pltpu.HBM) for x in operands])

    return jax.shard_map(
        step,
        mesh=mesh,
        in_specs=(P("rows", "section"), P("rows"), P(), P()),
        out_specs=P("rows", "section"),
        check_vma=False,
    )
```

```python
import functools

import jax
import jax.numpy as jnp
from jax import lax
from jax.experimental import pallas as pl
from jax.experimental.pallas import tpu as pltpu
from jax.sharding import PartitionSpec as P

CHUNKS = 4
PLANE = 4
RAW = 4
LINES = 4
GROUP = 8
TERMS = 2
F32 = jnp.float32
BF16 = jnp.bfloat16
I32 = jnp.int32


def split(x, terms):
    parts = []
    for _ in range(terms):
        part = x.astype(BF16)
        parts.append(part)
        x = x - part.astype(F32)
    return parts


def butterfly(
    n, table_hbm, mask_hbm, w_hbm, bias_hbm, out_ref,
    table_ref, mask_ref, bias_ref,
    tally, planes, prefix, raw, hold, came, joined, w_ref, wcat,
    send_sem, recv_sem, raw_send, raw_recv, count_send, count_recv, plane_send, plane_recv, load_sem,
):
    half, height = table_hbm.shape
    width = out_ref.shape[1]
    lines = height // 128
    levels = (n - 1).bit_length()
    lanes = height // CHUNKS
    side = min(PLANE, n)
    crowd = min(RAW, n)
    first = (crowd - 1).bit_length()
    count_planes = n // side
    me = lax.axis_index("rows")
    core = lax.axis_index("section")
    plane = me // side
    seat = lax.rem(me, side)

    columns = pl.ds(pl.multiple_of(core * width, 128), width)
    mask_copy = pltpu.make_async_copy(mask_hbm, mask_ref, load_sem.at[0])
    table_copy = pltpu.make_async_copy(table_hbm, table_ref, load_sem.at[1])
    w_copy = pltpu.make_async_copy(w_hbm.at[:, columns], w_ref, load_sem.at[2])
    bias_copy = pltpu.make_async_copy(bias_hbm.at[:, columns], bias_ref, load_sem.at[3])
    for load in (mask_copy, table_copy, w_copy, bias_copy):
        load.start()

    def seat_peer(step):
        return plane * side + lax.rem(seat + step, side)

    def plane_peer(step):
        return lax.rem(plane + step, count_planes) * side + seat

    barrier = pltpu.get_barrier_semaphore()
    for step in range(1, side):
        pl.semaphore_signal(barrier, inc=1, device_id={"rows": seat_peer(step)})
    for step in range(1, count_planes):
        pl.semaphore_signal(barrier, inc=1, device_id={"rows": plane_peer(step)})
    pl.semaphore_signal(barrier, inc=1, device_id={"section": 1 - core})

    mask_copy.wait()
    mask = mask_ref[...]
    ones = mask.astype(F32).astype(BF16)
    row = lax.broadcasted_iota(I32, (128, 128), 0)
    col = lax.broadcasted_iota(I32, (128, 128), 1)
    before = jnp.where(row < col, 1.0, 0.0).astype(BF16)
    inner = jnp.dot(ones, before, preferred_element_type=F32).astype(I32)
    sums = jnp.dot(ones, jnp.ones((128, 128), BF16), preferred_element_type=F32).astype(I32)
    running = jnp.zeros((1, 128), I32)
    starts = []
    for line in range(lines):
        starts.append(running)
        running = running + sums[line : line + 1]
    tally[seat] = running
    slot = jnp.where(mask == 1, inner + jnp.concatenate(starts, 0), -1)

    own = lax.rem(me, crowd)
    table_copy.wait()
    turned = jnp.concatenate(split(table_ref[...], 3), 0)
    for chunk in range(CHUNKS):
        here = chunk * lanes + lax.broadcasted_iota(I32, (lanes, 128), 0)
        hot = jnp.concatenate(
            [jnp.where(here == slot[b : b + 1], 1.0, 0.0).astype(BF16) for b in range(chunk * lanes // 128, lines)], 1
        )
        folded = lax.dot_general(
            turned[:, chunk * lanes :], hot, (((1,), (1,)), ((), ())), preferred_element_type=F32
        )
        raw[own, :, chunk * lanes : (chunk + 1) * lanes] = (
            folded[:half] + folded[half : 2 * half]
        ) + folded[2 * half :]

    pl.semaphore_wait(barrier, side + count_planes - 1)

    def seat_copy(step):
        return pltpu.make_async_remote_copy(
            src_ref=tally.at[seat], dst_ref=tally.at[seat],
            send_sem=count_send.at[step], recv_sem=count_recv.at[step],
            device_id={"rows": seat_peer(step)},
        )

    def plane_copy(step):
        return pltpu.make_async_remote_copy(
            src_ref=planes.at[plane], dst_ref=planes.at[plane],
            send_sem=plane_send.at[step], recv_sem=plane_recv.at[step],
            device_id={"rows": plane_peer(step)},
        )

    def raw_copy(step):
        return pltpu.make_async_remote_copy(
            src_ref=raw.at[own], dst_ref=raw.at[own],
            send_sem=raw_send.at[step], recv_sem=raw_recv.at[step],
            device_id={"rows": me - own + lax.rem(own + step, crowd)},
        )

    for step in range(1, side):
        seat_copy(step).start()
    for step in range(1, crowd):
        raw_copy(step).start()
    for step in range(1, side):
        seat_copy(step).wait_recv()
    everyone = jnp.zeros((1, 128), I32)
    for at in range(side):
        everyone = everyone + tally[at]
    planes[plane] = everyone
    for step in range(1, count_planes):
        plane_copy(step).start()

    w_copy.wait()
    bias_copy.wait()
    bias = bias_ref[...]
    w_hi, w_lo = split(w_ref[...], 2)
    b_hi, b_mid, b_lo = [part.astype(F32) for part in split(bias, 3)]
    line = lax.broadcasted_iota(I32, (16, width), 0)
    extra = jnp.where(line == 0, b_hi, jnp.where(line == 1, b_mid, jnp.where(line == 2, b_lo, 0.0)))
    wcat[...] = jnp.concatenate([w_hi, w_lo, w_hi, extra.astype(BF16)], 0)

    for step in range(1, count_planes):
        plane_copy(step).wait_recv()
    total = jnp.zeros((1, 128), I32)
    for at in range(count_planes):
        prefix[at * side] = total
        total = total + planes[at]
    prefix[n] = total
    running = prefix[plane * side]
    for at in range(side - 1):
        running = running + tally[at]
        prefix[plane * side + at + 1] = running

    def wide(x):
        return jnp.concatenate([x] * (lanes // 128), 1)

    def data_copy(level, chunk):
        at = (slice(None), pl.ds(chunk * lanes, lanes))
        return pltpu.make_async_remote_copy(
            src_ref=hold.at[(level,) + at], dst_ref=came.at[(level,) + at],
            send_sem=send_sem.at[level, chunk], recv_sem=recv_sem.at[level, chunk],
            device_id={"rows": me + (1 - 2 * (me // (1 << level) % 2)) * (1 << level)},
        )

    def join_copy(chunk):
        at = (core, slice(None), pl.ds(chunk * lanes, lanes))
        return pltpu.make_async_remote_copy(
            src_ref=joined.at[at], dst_ref=joined.at[at],
            send_sem=send_sem.at[levels, chunk], recv_sem=recv_sem.at[levels, chunk],
            device_id={"section": 1 - core},
        )

    for step in range(1, crowd):
        raw_copy(step).wait_recv()
    turns = []
    for at in range(crowd):
        shift = (prefix[me - own + at] & (height - 1))[0, 0]
        turns.append(pltpu.roll(raw[at], shift, 1))
    low = wide(prefix[me - own])
    for chunk in range(CHUNKS):
        at = slice(chunk * lanes, (chunk + 1) * lanes)
        base = own * height + chunk * lanes + lax.broadcasted_iota(I32, (1, lanes), 1)
        place = low + ((base - low) & (crowd * height - 1))
        place = jnp.broadcast_to(place, (half, lanes))
        block = turns[0][:, at]
        for other in range(1, crowd):
            block = jnp.where(place >= wide(prefix[me - own + other]), turns[other][:, at], block)
        hold[first, :, at] = block
        data_copy(first, chunk).start()

    for level in range(first, levels):
        reach = 2 << level
        group = me // reach * reach
        bit = me // (1 << level) % 2
        low = wide(prefix[group])
        middle = wide(prefix[group + (1 << level)])
        for chunk in range(CHUNKS):
            at = slice(chunk * lanes, (chunk + 1) * lanes)
            data_copy(level, chunk).wait_recv()
            base = (me % reach) * height + chunk * lanes
            base = base + lax.broadcasted_iota(I32, (1, lanes), 1)
            place = low + ((base - low) & (reach * height - 1))
            upper = jnp.where(place >= middle, 1, 0)
            foreign = jnp.broadcast_to(upper, (half, lanes)) != bit
            block = jnp.where(foreign, came[level, :, at], hold[level, :, at])
            if level < levels - 1:
                hold[level + 1, :, at] = block
                data_copy(level + 1, chunk).start()
            else:
                joined[core, :, at] = block
                join_copy(chunk).start()

    ends = wide(total)
    for chunk in range(CHUNKS):
        at = slice(chunk * lanes, (chunk + 1) * lanes)
        join_copy(chunk).wait_recv()
        owned = me * height + chunk * lanes + lax.broadcasted_iota(I32, (1, lanes), 1)
        filled = jnp.where(owned < ends, 1.0, 0.0)
        rows = jnp.concatenate([joined[0, :, at], joined[1, :, at]], 0)
        rows = jnp.where(jnp.broadcast_to(filled, rows.shape) > 0.5, rows, 0.0)
        a_hi, a_lo = split(rows, 2)
        marks = jnp.broadcast_to(filled, (16, lanes)).astype(BF16)
        lhs = jnp.concatenate([a_hi, a_hi, a_lo, marks], 0)
        out_ref[at, :] = lax.dot_general(
            lhs, wcat[...], (((0,), (0,)), ((), ())), preferred_element_type=F32
        ).astype(BF16)

    for step in range(1, side):
        seat_copy(step).wait_send()
    for step in range(1, count_planes):
        plane_copy(step).wait_send()
    for step in range(1, crowd):
        raw_copy(step).wait_send()
    for level in range(first, levels):
        for chunk in range(CHUNKS):
            data_copy(level, chunk).wait_send()
    for chunk in range(CHUNKS):
        join_copy(chunk).wait_send()


def wide(x, lanes):
    return jnp.concatenate([x] * (lanes // 128), 1)


def flip(at, step, extent):
    out, bit = 0, 1
    while bit < extent:
        a, b = at // bit % 2, step // bit % 2
        out = out + bit * (a + b - 2 * a * b)
        bit *= 2
    return out


def direct(
    n, table_hbm, mask_hbm, w_hbm, bias_hbm, out_ref,
    table_ref, mask_ref, bias_ref,
    tally, prefix, gather, pieces, got, joined, w_ref, wcat,
    load_sem, count_send, count_recv, gather_send, gather_recv,
    piece_send, piece_recv, across_send, across_recv, join_send, join_recv,
):
    half, height = table_hbm.shape
    width = out_ref.shape[1]
    rows = height // 128
    lanes = height // CHUNKS
    groups = half // GROUP
    side = min(PLANE, n)
    lines = n // side
    me = lax.axis_index("rows")
    core = lax.axis_index("section")
    line = me // side
    seat = lax.rem(me, side)
    flat = core == 1

    columns = pl.ds(pl.multiple_of(core * width, 128), width)
    mask_copy = pltpu.make_async_copy(mask_hbm, mask_ref, load_sem.at[0])
    table_copy = pltpu.make_async_copy(table_hbm, table_ref, load_sem.at[1])
    w_copy = pltpu.make_async_copy(w_hbm.at[:, columns], w_ref, load_sem.at[2])
    bias_copy = pltpu.make_async_copy(bias_hbm.at[:, columns], bias_ref, load_sem.at[3])
    for load in (mask_copy, table_copy, w_copy, bias_copy):
        load.start()

    barrier = pltpu.get_barrier_semaphore()
    pl.semaphore_signal(barrier, inc=1, device_id={"section": 1 - core})

    @pl.when(flat)
    def _():
        for step in range(1, n):
            pl.semaphore_signal(barrier, inc=1, device_id={"rows": lax.rem(me + step, n)})

    @pl.when(core == 0)
    def _():
        for step in range(1, side):
            pl.semaphore_signal(barrier, inc=1, device_id={"rows": line * side + flip(seat, step, side)})
        for other in range(1, lines):
            @pl.when(line < other)
            def _(other=other):
                pl.semaphore_signal(barrier, inc=1, device_id={"rows": other * side + seat})

    mask_copy.wait()
    mask = mask_ref[...]
    ones = mask.astype(F32).astype(BF16)
    row = lax.broadcasted_iota(I32, (128, 128), 0)
    col = lax.broadcasted_iota(I32, (128, 128), 1)
    before = jnp.where(row < col, 1.0, 0.0).astype(BF16)
    inner = jnp.dot(ones, before, preferred_element_type=F32).astype(I32)
    sums = jnp.dot(ones, jnp.ones((128, 128), BF16), preferred_element_type=F32).astype(I32)
    running = jnp.zeros((1, 128), I32)
    starts = []
    for at in range(rows):
        starts.append(running)
        running = running + sums[at : at + 1]
    tally[me] = running
    slot = jnp.where(mask == 1, inner + jnp.concatenate(starts, 0), -1)

    own = jnp.where(flat, seat, line)
    table_copy.wait()
    terms = jnp.concatenate(split(table_ref[...], TERMS), 0)
    for chunk in range(CHUNKS):
        here = chunk * lanes + lax.broadcasted_iota(I32, (lanes, 128), 0)
        hot = jnp.concatenate(
            [jnp.where(here == slot[b : b + 1], 1.0, 0.0).astype(BF16) for b in range(chunk * lanes // 128, rows)], 1
        )
        folded = lax.dot_general(
            terms[:, chunk * lanes :], hot, (((1,), (1,)), ((), ())), preferred_element_type=F32
        )
        block = folded[:half]
        for term in range(1, TERMS):
            block = block + folded[term * half : (term + 1) * half]
        gather[own, :, chunk * lanes : (chunk + 1) * lanes] = block

    def span(g):
        return pl.ds(g * GROUP, GROUP)

    def remote(src, dst, send, recv, **to):
        return pltpu.make_async_remote_copy(src_ref=src, dst_ref=dst, send_sem=send, recv_sem=recv, device_id=to)

    def blocks_of(count, g):
        return gather.at[pl.ds(0, count), span(g)]

    def count_copy(step):
        return remote(tally.at[me], tally.at[me], count_send.at[0], count_recv.at[0], rows=lax.rem(me + step, n))

    def prefix_copy():
        return remote(prefix, prefix, count_send.at[1], count_recv.at[1], section=1 - core)

    def seat_copy(step, g):
        at = gather.at[seat, span(g)]
        to = line * side + flip(seat, step, side)
        return remote(at, at, gather_send.at[0], gather_recv.at[g], rows=to)

    def line_copy(source, target, g):
        at = gather.at[source, span(g)]
        return remote(at, at, gather_send.at[0], gather_recv.at[g], rows=target * side + seat)

    def down_copy(source, target, g):
        return remote(
            pieces.at[target, span(g)], got.at[source, span(g)],
            piece_send.at[0], piece_recv.at[g], rows=target * side + seat,
        )

    def across_copy(step, g):
        return remote(
            pieces.at[step, span(g)], got.at[step, span(g)],
            across_send.at[0], across_recv.at[g], rows=line * side + flip(seat, step, side),
        )

    def join_copy(g):
        at = joined.at[core, span(g)]
        return remote(at, at, join_send.at[0], join_recv.at[0], section=1 - core)

    def arrived(count, g, sem):
        at = blocks_of(count, g)
        remote(at, at, sem, sem, section=core).wait_recv()

    def left(count, sem):
        for at in range(0, count, side):
            some = gather.at[pl.ds(0, min(side, count - at))]
            remote(some, some, sem, sem, section=core).wait_send()

    pl.semaphore_wait(barrier, jnp.where(flat, n, side + line))

    @pl.when(flat)
    def _():
        for step in range(1, n):
            count_copy(step).start()
        for g in range(groups):
            for step in range(1, side):
                seat_copy(step, g).start()

    for source in range(1, lines):
        @pl.when(jnp.logical_and(core == 0, line == source))
        def _(source=source):
            for target in range(source):
                for g in range(groups):
                    line_copy(source, target, g).start()

    w_copy.wait()
    bias_copy.wait()
    bias = bias_ref[...]
    w_hi, w_lo = split(w_ref[...], 2)
    b_hi, b_mid, b_lo = [part.astype(F32) for part in split(bias, 3)]
    at = lax.broadcasted_iota(I32, (16, width), 0)
    extra = jnp.where(at == 0, b_hi, jnp.where(at == 1, b_mid, jnp.where(at == 2, b_lo, 0.0)))
    wcat[...] = jnp.concatenate([w_hi, w_lo, w_hi, extra.astype(BF16)], 0)

    lane = lax.broadcasted_iota(I32, (GROUP, height), 1)

    def bound(index):
        return wide(jnp.broadcast_to(prefix[index], (GROUP, 128)), height)

    def turn(slot, index, g):
        shift = (prefix[index] & (height - 1))[0, 0]
        return pltpu.roll(gather[slot, g * GROUP : (g + 1) * GROUP], shift, 1)

    @pl.when(flat)
    def _():
        others = tally.at[pl.ds(0, n - 1)]
        remote(others, others, count_send.at[0], count_recv.at[0], section=core).wait_recv()
        total = jnp.zeros((1, 128), I32)
        for at in range(n):
            prefix[at] = total
            total = total + tally[at]
        prefix[n] = total
        prefix_copy().start()

        for z in range(lines):
            @pl.when(line == z)
            def _(z=z):
                base = seat * height + lane
                low, high = bound(z * side), bound(z * side + side)
                relayed = lines > 3 and z == 3
                for g in range(groups):
                    at_g = slice(g * GROUP, (g + 1) * GROUP)
                    arrived(side - 1, g, gather_recv.at[g])
                    blocks = [turn(at, z * side + at, g) for at in range(side)]

                    def choose(place):
                        piece = jnp.where(place >= low, blocks[0], 0.0)
                        for at in range(1, side):
                            piece = jnp.where(place >= bound(z * side + at), blocks[at], piece)
                        return jnp.where(place >= high, 0.0, piece)

                    if relayed:
                        place = low + ((base - low) & (side * height - 1))
                        mixed = choose(place)
                        pieces[2, at_g] = mixed
                        down_copy(3, 2, g).start()
                        joined[1, at_g] = jnp.where(place >= 3 * side * height, mixed, 0.0)
                    else:
                        for target in range(z):
                            pieces[target, at_g] = choose(target * side * height + base)
                            if not (lines > 3 and z == 2):
                                down_copy(z, target, g).start()
                        joined[1, at_g] = choose(z * side * height + base)
                if lines > 3 and z == 2:
                    top = bound(4 * side)
                    for g in range(groups):
                        at_g = slice(g * GROUP, (g + 1) * GROUP)
                        arrived(1, g, piece_recv.at[g])
                        for target in range(2):
                            place = target * side * height + base
                            inside = jnp.logical_and(place >= high, place < top)
                            pieces[target, at_g] = jnp.where(inside, got[3, at_g], pieces[target, at_g])
                            if target == 0:
                                down_copy(2, 0, g).start()
                        place = 2 * side * height + base
                        inside = jnp.logical_and(place >= high, place < top)
                        joined[1, at_g] = jnp.where(inside, got[3, at_g], joined[1, at_g])
                        join_copy(g).start()
                    for g in range(groups):
                        down_copy(2, 1, g).start()
                else:
                    sources = range(z + 1, min(lines, 3))
                    for g in range(groups):
                        at_g = slice(g * GROUP, (g + 1) * GROUP)
                        if sources:
                            arrived(len(sources), g, piece_recv.at[g])
                            block = joined[1, at_g]
                            for source in sources:
                                block = block + got[source, at_g]
                            joined[1, at_g] = block
                        join_copy(g).start()

    @pl.when(core == 0)
    def _():
        prefix_copy().wait_recv()
        for z in range(lines):
            @pl.when(line == z)
            def _(z=z):
                sources = range(z, lines)
                for g in range(groups):
                    at_g = slice(g * GROUP, (g + 1) * GROUP)
                    if z + 1 < lines:
                        arrived(lines - 1 - z, g, gather_recv.at[g])
                    blocks = [turn(at, at * side + seat, g) for at in sources]
                    for step in [*range(1, side), 0]:
                        place = (z * side + flip(seat, step, side)) * height + lane
                        piece = jnp.zeros((GROUP, height), F32)
                        for at, block in zip(sources, blocks):
                            index = at * side + seat
                            inside = jnp.logical_and(place >= bound(index), place < bound(index + 1))
                            piece = jnp.where(inside, block, piece)
                        if step:
                            pieces[step, at_g] = piece
                            across_copy(step, g).start()
                        else:
                            joined[0, at_g] = piece
        for g in range(groups):
            at_g = slice(g * GROUP, (g + 1) * GROUP)
            arrived(side - 1, g, across_recv.at[g])
            block = joined[0, at_g]
            for step in range(1, side):
                block = block + got[step, at_g]
            joined[0, at_g] = block
            join_copy(g).start()

    other = joined.at[1 - core]
    remote(other, other, join_send.at[0], join_recv.at[0], section=1 - core).wait_recv()
    ends = wide(prefix[n], lanes)
    for chunk in range(CHUNKS):
        at = slice(chunk * lanes, (chunk + 1) * lanes)
        owned = me * height + chunk * lanes + lax.broadcasted_iota(I32, (1, lanes), 1)
        filled = jnp.where(owned < ends, 1.0, 0.0)
        block = jnp.concatenate([joined[0, :, at], joined[1, :, at]], 0)
        a_hi, a_lo = split(block, 2)
        marks = jnp.broadcast_to(filled, (16, lanes)).astype(BF16)
        lhs = jnp.concatenate([a_hi, a_hi, a_lo, marks], 0)
        out_ref[at, :] = lax.dot_general(
            lhs, wcat[...], (((0,), (0,)), ((), ())), preferred_element_type=F32
        ).astype(BF16)

    left(1, join_send.at[0])

    @pl.when(flat)
    def _():
        others = tally.at[pl.ds(0, n - 1)]
        remote(others, others, count_send.at[0], count_recv.at[0], section=core).wait_send()
        prefix_copy().wait_send()
        left(side - 1, gather_send.at[0])

    for z in range(1, lines):
        @pl.when(jnp.logical_and(flat, line == z))
        def _(z=z):
            left(1 if lines > 3 and z == 3 else z, piece_send.at[0])

        @pl.when(jnp.logical_and(core == 0, line == z))
        def _(z=z):
            left(z, gather_send.at[0])

    @pl.when(core == 0)
    def _():
        left(side - 1, across_send.at[0])


def solution(mesh):
    n, sections = mesh.shape["rows"], mesh.shape["section"]

    def step(table, mask, weight, bias):
        height, half = table.shape
        cols, features = weight.shape
        width = features // sections
        levels = (n - 1).bit_length()
        side, crowd = min(PLANE, n), min(RAW, n)
        lines, groups = n // side, half // GROUP
        operands = table.T, mask.reshape(height // 128, 128), weight, bias.reshape(1, features)
        sem = pltpu.SemaphoreType.DMA
        loads = [
            pltpu.VMEM((half, height), F32),
            pltpu.VMEM((height // 128, 128), I32),
            pltpu.VMEM((1, width), F32),
        ]
        weights = [
            pltpu.VMEM((cols, width), F32),
            pltpu.VMEM((3 * cols + 16, width), BF16),
        ]
        if lines <= LINES:
            most = max(side, lines)
            block = pltpu.VMEM((most, half, height), F32)
            body = direct
            scratch = loads + [
                pltpu.VMEM((n, 1, 128), I32),
                pltpu.VMEM((n + 1, 1, 128), I32),
                block, block, block,
                pltpu.VMEM((sections, half, height), F32),
            ] + weights + [
                sem((4,)), sem((2,)), sem((2,)),
                sem((1,)), sem((groups,)),
                sem((1,)), sem((groups,)), sem((1,)), sem((groups,)),
                sem((1,)), sem((1,)),
            ]
        else:
            body = butterfly
            scratch = loads + [
                pltpu.VMEM((side, 1, 128), I32),
                pltpu.VMEM((n // side, 1, 128), I32),
                pltpu.VMEM((n + 1, 1, 128), I32),
                pltpu.VMEM((crowd, half, height), F32),
                pltpu.VMEM((levels, half, height), F32),
                pltpu.VMEM((levels, half, height), F32),
                pltpu.VMEM((sections, half, height), F32),
            ] + weights + [
                sem((levels + 1, CHUNKS)), sem((levels + 1, CHUNKS)),
                sem((crowd,)), sem((crowd,)),
                sem((side,)), sem((side,)),
                sem((n // side,)), sem((n // side,)),
                sem((4,)),
            ]
        return pl.pallas_call(
            functools.partial(body, n),
            name="filter_project",
            out_shape=jax.ShapeDtypeStruct((height, width), BF16),
            in_specs=[pl.BlockSpec(memory_space=pltpu.HBM)] * 4,
            out_specs=pl.BlockSpec(memory_space=pltpu.VMEM),
            scratch_shapes=scratch,
            compiler_params=pltpu.CompilerParams(
                collective_id=0, has_side_effects=True, vmem_limit_bytes=16 << 20
            ),
        )(*[pltpu.with_memory_space_constraint(x, pltpu.HBM) for x in operands])

    return jax.shard_map(
        step,
        mesh=mesh,
        in_specs=(P("rows", "section"), P("rows"), P(), P()),
        out_specs=P("rows", "section"),
        check_vma=False,
    )
```

```python
import functools

import jax
import jax.numpy as jnp
from jax import lax
from jax.experimental import pallas as pl
from jax.experimental.pallas import tpu as pltpu
from jax.sharding import PartitionSpec as P

CHUNKS = 4
PLANE = 4
RAW = 4
LINES = 4
GROUP = 8
TERMS = 2
MERGE = 2
EARLY = 1
F32 = jnp.float32
BF16 = jnp.bfloat16
I32 = jnp.int32


def split(x, terms):
    parts = []
    for _ in range(terms):
        part = x.astype(BF16)
        parts.append(part)
        x = x - part.astype(F32)
    return parts


def butterfly(
    n, table_hbm, mask_hbm, w_hbm, bias_hbm, out_ref,
    table_ref, mask_ref, bias_ref,
    tally, planes, prefix, raw, hold, came, joined, w_ref, wcat,
    send_sem, recv_sem, raw_send, raw_recv, count_send, count_recv, plane_send, plane_recv, load_sem,
):
    half, height = table_hbm.shape
    width = out_ref.shape[1]
    lines = height // 128
    levels = (n - 1).bit_length()
    lanes = height // CHUNKS
    side = min(PLANE, n)
    crowd = min(RAW, n)
    first = (crowd - 1).bit_length()
    count_planes = n // side
    me = lax.axis_index("rows")
    core = lax.axis_index("section")
    plane = me // side
    seat = lax.rem(me, side)

    columns = pl.ds(pl.multiple_of(core * width, 128), width)
    mask_copy = pltpu.make_async_copy(mask_hbm, mask_ref, load_sem.at[0])
    table_copy = pltpu.make_async_copy(table_hbm, table_ref, load_sem.at[1])
    w_copy = pltpu.make_async_copy(w_hbm.at[:, columns], w_ref, load_sem.at[2])
    bias_copy = pltpu.make_async_copy(bias_hbm.at[:, columns], bias_ref, load_sem.at[3])
    for load in (mask_copy, table_copy, w_copy, bias_copy):
        load.start()

    def seat_peer(step):
        return plane * side + lax.rem(seat + step, side)

    def plane_peer(step):
        return lax.rem(plane + step, count_planes) * side + seat

    barrier = pltpu.get_barrier_semaphore()
    for step in range(1, side):
        pl.semaphore_signal(barrier, inc=1, device_id={"rows": seat_peer(step)})
    for step in range(1, count_planes):
        pl.semaphore_signal(barrier, inc=1, device_id={"rows": plane_peer(step)})
    pl.semaphore_signal(barrier, inc=1, device_id={"section": 1 - core})

    mask_copy.wait()
    mask = mask_ref[...]
    ones = mask.astype(F32).astype(BF16)
    row = lax.broadcasted_iota(I32, (128, 128), 0)
    col = lax.broadcasted_iota(I32, (128, 128), 1)
    before = jnp.where(row < col, 1.0, 0.0).astype(BF16)
    inner = jnp.dot(ones, before, preferred_element_type=F32).astype(I32)
    sums = jnp.dot(ones, jnp.ones((128, 128), BF16), preferred_element_type=F32).astype(I32)
    running = jnp.zeros((1, 128), I32)
    starts = []
    for line in range(lines):
        starts.append(running)
        running = running + sums[line : line + 1]
    tally[seat] = running
    slot = jnp.where(mask == 1, inner + jnp.concatenate(starts, 0), -1)

    own = lax.rem(me, crowd)
    table_copy.wait()
    turned = jnp.concatenate(split(table_ref[...], 3), 0)
    for chunk in range(CHUNKS):
        here = chunk * lanes + lax.broadcasted_iota(I32, (lanes, 128), 0)
        hot = jnp.concatenate(
            [jnp.where(here == slot[b : b + 1], 1.0, 0.0).astype(BF16) for b in range(chunk * lanes // 128, lines)], 1
        )
        folded = lax.dot_general(
            turned[:, chunk * lanes :], hot, (((1,), (1,)), ((), ())), preferred_element_type=F32
        )
        raw[own, :, chunk * lanes : (chunk + 1) * lanes] = (
            folded[:half] + folded[half : 2 * half]
        ) + folded[2 * half :]

    pl.semaphore_wait(barrier, side + count_planes - 1)

    def seat_copy(step):
        return pltpu.make_async_remote_copy(
            src_ref=tally.at[seat], dst_ref=tally.at[seat],
            send_sem=count_send.at[step], recv_sem=count_recv.at[step],
            device_id={"rows": seat_peer(step)},
        )

    def plane_copy(step):
        return pltpu.make_async_remote_copy(
            src_ref=planes.at[plane], dst_ref=planes.at[plane],
            send_sem=plane_send.at[step], recv_sem=plane_recv.at[step],
            device_id={"rows": plane_peer(step)},
        )

    def raw_copy(step):
        return pltpu.make_async_remote_copy(
            src_ref=raw.at[own], dst_ref=raw.at[own],
            send_sem=raw_send.at[step], recv_sem=raw_recv.at[step],
            device_id={"rows": me - own + lax.rem(own + step, crowd)},
        )

    for step in range(1, side):
        seat_copy(step).start()
    for step in range(1, crowd):
        raw_copy(step).start()
    for step in range(1, side):
        seat_copy(step).wait_recv()
    everyone = jnp.zeros((1, 128), I32)
    for at in range(side):
        everyone = everyone + tally[at]
    planes[plane] = everyone
    for step in range(1, count_planes):
        plane_copy(step).start()

    w_copy.wait()
    bias_copy.wait()
    bias = bias_ref[...]
    w_hi, w_lo = split(w_ref[...], 2)
    b_hi, b_mid, b_lo = [part.astype(F32) for part in split(bias, 3)]
    line = lax.broadcasted_iota(I32, (16, width), 0)
    extra = jnp.where(line == 0, b_hi, jnp.where(line == 1, b_mid, jnp.where(line == 2, b_lo, 0.0)))
    wcat[...] = jnp.concatenate([w_hi, w_lo, w_hi, extra.astype(BF16)], 0)

    for step in range(1, count_planes):
        plane_copy(step).wait_recv()
    total = jnp.zeros((1, 128), I32)
    for at in range(count_planes):
        prefix[at * side] = total
        total = total + planes[at]
    prefix[n] = total
    running = prefix[plane * side]
    for at in range(side - 1):
        running = running + tally[at]
        prefix[plane * side + at + 1] = running

    def wide(x):
        return jnp.concatenate([x] * (lanes // 128), 1)

    def data_copy(level, chunk):
        at = (slice(None), pl.ds(chunk * lanes, lanes))
        return pltpu.make_async_remote_copy(
            src_ref=hold.at[(level,) + at], dst_ref=came.at[(level,) + at],
            send_sem=send_sem.at[level, chunk], recv_sem=recv_sem.at[level, chunk],
            device_id={"rows": me + (1 - 2 * (me // (1 << level) % 2)) * (1 << level)},
        )

    def join_copy(chunk):
        at = (core, slice(None), pl.ds(chunk * lanes, lanes))
        return pltpu.make_async_remote_copy(
            src_ref=joined.at[at], dst_ref=joined.at[at],
            send_sem=send_sem.at[levels, chunk], recv_sem=recv_sem.at[levels, chunk],
            device_id={"section": 1 - core},
        )

    for step in range(1, crowd):
        raw_copy(step).wait_recv()
    turns = []
    for at in range(crowd):
        shift = (prefix[me - own + at] & (height - 1))[0, 0]
        turns.append(pltpu.roll(raw[at], shift, 1))
    low = wide(prefix[me - own])
    for chunk in range(CHUNKS):
        at = slice(chunk * lanes, (chunk + 1) * lanes)
        base = own * height + chunk * lanes + lax.broadcasted_iota(I32, (1, lanes), 1)
        place = low + ((base - low) & (crowd * height - 1))
        place = jnp.broadcast_to(place, (half, lanes))
        block = turns[0][:, at]
        for other in range(1, crowd):
            block = jnp.where(place >= wide(prefix[me - own + other]), turns[other][:, at], block)
        hold[first, :, at] = block
        data_copy(first, chunk).start()

    for level in range(first, levels):
        reach = 2 << level
        group = me // reach * reach
        bit = me // (1 << level) % 2
        low = wide(prefix[group])
        middle = wide(prefix[group + (1 << level)])
        for chunk in range(CHUNKS):
            at = slice(chunk * lanes, (chunk + 1) * lanes)
            data_copy(level, chunk).wait_recv()
            base = (me % reach) * height + chunk * lanes
            base = base + lax.broadcasted_iota(I32, (1, lanes), 1)
            place = low + ((base - low) & (reach * height - 1))
            upper = jnp.where(place >= middle, 1, 0)
            foreign = jnp.broadcast_to(upper, (half, lanes)) != bit
            block = jnp.where(foreign, came[level, :, at], hold[level, :, at])
            if level < levels - 1:
                hold[level + 1, :, at] = block
                data_copy(level + 1, chunk).start()
            else:
                joined[core, :, at] = block
                join_copy(chunk).start()

    ends = wide(total)
    for chunk in range(CHUNKS):
        at = slice(chunk * lanes, (chunk + 1) * lanes)
        join_copy(chunk).wait_recv()
        owned = me * height + chunk * lanes + lax.broadcasted_iota(I32, (1, lanes), 1)
        filled = jnp.where(owned < ends, 1.0, 0.0)
        rows = jnp.concatenate([joined[0, :, at], joined[1, :, at]], 0)
        rows = jnp.where(jnp.broadcast_to(filled, rows.shape) > 0.5, rows, 0.0)
        a_hi, a_lo = split(rows, 2)
        marks = jnp.broadcast_to(filled, (16, lanes)).astype(BF16)
        lhs = jnp.concatenate([a_hi, a_hi, a_lo, marks], 0)
        out_ref[at, :] = lax.dot_general(
            lhs, wcat[...], (((0,), (0,)), ((), ())), preferred_element_type=F32
        ).astype(BF16)

    for step in range(1, side):
        seat_copy(step).wait_send()
    for step in range(1, count_planes):
        plane_copy(step).wait_send()
    for step in range(1, crowd):
        raw_copy(step).wait_send()
    for level in range(first, levels):
        for chunk in range(CHUNKS):
            data_copy(level, chunk).wait_send()
    for chunk in range(CHUNKS):
        join_copy(chunk).wait_send()


def wide(x, lanes):
    return jnp.concatenate([x] * (lanes // 128), 1)


def flip(at, step, extent):
    out, bit = 0, 1
    while bit < extent:
        a, b = at // bit % 2, step // bit % 2
        out = out + bit * (a + b - 2 * a * b)
        bit *= 2
    return out


def direct(
    n, table_hbm, mask_hbm, w_hbm, bias_hbm, out_ref,
    table_ref, mask_ref, bias_ref,
    tally, prefix, gather, heap, pieces, parts, got, came, joined, w_ref, wcat,
    load_sem, count_send, count_recv, line_recv, gather_send, gather_recv, heap_recv,
    piece_send, piece_recv, across_send, across_recv, join_send, join_recv,
):
    half, height = table_hbm.shape
    width = out_ref.shape[1]
    rows = height // 128
    lanes = height // CHUNKS
    groups = half // GROUP
    side = min(PLANE, n)
    lines = n // side
    me = lax.axis_index("rows")
    core = lax.axis_index("section")
    line = me // side
    seat = lax.rem(me, side)
    flat = core == 1

    columns = pl.ds(pl.multiple_of(core * width, 128), width)
    mask_copy = pltpu.make_async_copy(mask_hbm, mask_ref, load_sem.at[0])
    table_copy = pltpu.make_async_copy(table_hbm, table_ref, load_sem.at[1])
    w_copy = pltpu.make_async_copy(w_hbm.at[:, columns], w_ref, load_sem.at[2])
    bias_copy = pltpu.make_async_copy(bias_hbm.at[:, columns], bias_ref, load_sem.at[3])
    for load in (mask_copy, table_copy, w_copy, bias_copy):
        load.start()

    barrier = pltpu.get_barrier_semaphore()
    pl.semaphore_signal(barrier, inc=1, device_id={"section": 1 - core})

    def tells(source, target):
        return source != target and not (source == 0 and target > 1)

    def far(source, target):
        return source > 1 and target == 0

    @pl.when(flat)
    def _():
        for step in range(1, side):
            pl.semaphore_signal(barrier, inc=1, device_id={"rows": line * side + flip(seat, step, side)})
        for other in range(lines):
            for z in range(lines):
                if tells(other, z):
                    @pl.when(line == z)
                    def _(other=other):
                        pl.semaphore_signal(barrier, inc=1, device_id={"rows": other * side + seat})
            for z in range(other):
                @pl.when(line == z)
                def _(other=other, z=z):
                    for at in range(side) if far(other, z) else [seat]:
                        pl.semaphore_signal(barrier, inc=1, device_id={"rows": other * side + at, "section": 0})

    mask_copy.wait()
    mask = mask_ref[...]
    ones = mask.astype(F32).astype(BF16)
    row = lax.broadcasted_iota(I32, (128, 128), 0)
    col = lax.broadcasted_iota(I32, (128, 128), 1)
    before = jnp.where(row < col, 1.0, 0.0).astype(BF16)
    inner = jnp.dot(ones, before, preferred_element_type=F32).astype(I32)
    sums = jnp.dot(ones, jnp.ones((128, 128), BF16), preferred_element_type=F32).astype(I32)
    running = jnp.zeros((1, 128), I32)
    starts = []
    for at in range(rows):
        starts.append(running)
        running = running + sums[at : at + 1]
    tally[me] = running
    slot = jnp.where(mask == 1, inner + jnp.concatenate(starts, 0), -1)

    def far_count():
        at = tally.at[me]
        return [
            pltpu.make_async_remote_copy(
                src_ref=at, dst_ref=at, send_sem=count_send.at[1], recv_sem=count_recv.at[2],
                device_id={"rows": to, "section": 1},
            )
            for to in range(side)
        ]

    for z in range(lines):
        @pl.when(jnp.logical_and(core == 0, line == z))
        def _(z=z):
            pl.semaphore_wait(barrier, 1 + z + (side - 1 if z > 1 else 0))
            if z > 1:
                for copy in far_count():
                    copy.start()

    own = jnp.where(flat, seat, line)
    table_copy.wait()
    terms = jnp.concatenate(split(table_ref[...], TERMS), 0)
    for chunk in range(CHUNKS):
        here = chunk * lanes + lax.broadcasted_iota(I32, (lanes, 128), 0)
        hot = jnp.concatenate(
            [jnp.where(here == slot[b : b + 1], 1.0, 0.0).astype(BF16) for b in range(chunk * lanes // 128, rows)], 1
        )
        folded = lax.dot_general(
            terms[:, chunk * lanes :], hot, (((1,), (1,)), ((), ())), preferred_element_type=F32
        )
        block = folded[:half]
        for term in range(1, TERMS):
            block = block + folded[term * half : (term + 1) * half]
        gather[own, :, chunk * lanes : (chunk + 1) * lanes] = block

    def span(g):
        return pl.ds(g * GROUP, GROUP)

    def remote(src, dst, send, recv, **to):
        return pltpu.make_async_remote_copy(src_ref=src, dst_ref=dst, send_sem=send, recv_sem=recv, device_id=to)

    def seat_count():
        at = tally.at[me]
        return [
            remote(at, at, count_send.at[0], count_recv.at[0], rows=line * side + flip(seat, step, side))
            for step in range(1, side)
        ]

    def line_count(source, target):
        low = 0 if target > source == 1 else source * side
        at = tally.at[pl.ds(low, (source + 1) * side - low)]
        return remote(
            at, at, count_send.at[2 if target > source else 1], line_recv.at[source], rows=target * side + seat
        )

    def total_copy():
        at = prefix.at[n]
        return remote(at, at, count_send.at[3], count_recv.at[1], section=1 - core)

    def seat_copy(step, g):
        at = gather.at[seat, span(g)]
        to = line * side + flip(seat, step, side)
        return remote(at, at, gather_send.at[0], gather_recv.at[g], rows=to)

    def line_copy(source, target, g):
        return remote(
            gather.at[source, span(g)], heap.at[source, span(g)],
            gather_send.at[0], heap_recv.at[g], rows=target * side + seat, section=1,
        )

    def order(source):
        every = range(groups)
        first = [(0, g) for g in every] if source else []
        near = [(target, g) for target in reversed(range(2, source)) for g in every]
        after = [(source, g) for g in every] + [(1, g) for g in every if source > 1]
        return first[:EARLY] + near + first[EARLY:] + after

    def down_copy(source, target, g):
        return remote(
            pieces.at[target, span(g)], got.at[source, span(g)],
            piece_send.at[0], piece_recv.at[g], rows=target * side + seat,
        )

    def across_copy(step, g):
        return remote(
            parts.at[step, span(g)], came.at[step, span(g)],
            across_send.at[0], across_recv.at[g], rows=line * side + flip(seat, step, side),
        )

    def join_copy(which, g):
        at = joined.at[which, span(g)]
        return remote(at, at, join_send.at[0], join_recv.at[0], section=1 - core)

    def arrived(count, g, sem):
        at = heap.at[pl.ds(0, count), span(g)]
        remote(at, at, sem, sem, section=core).wait_recv()

    def left(count, sem):
        at = heap.at[pl.ds(0, count)]
        remote(at, at, sem, sem, section=core).wait_send()

    def told(count, sem):
        at = tally.at[pl.ds(0, count)]
        remote(at, at, sem, sem, section=core).wait_recv()

    def said(count, sem):
        at = tally.at[pl.ds(0, count)]
        remote(at, at, sem, sem, section=core).wait_send()

    def extend(start, stop):
        running = prefix[start] if start else jnp.zeros((1, 128), I32)
        prefix[start] = running
        for at in range(start, stop):
            running = running + tally[at]
            prefix[at + 1] = running

    for z in range(lines):
        ahead = sum(tells(z, other) for other in range(lines))
        @pl.when(jnp.logical_and(flat, line == z))
        def _(ahead=ahead):
            pl.semaphore_wait(barrier, side + ahead)

    @pl.when(flat)
    def _():
        for copy in seat_count():
            copy.start()
        for g in range(groups):
            for step in range(1, side):
                seat_copy(step, g).start()

    for source in range(lines):
        @pl.when(jnp.logical_and(core == 0, line == source))
        def _(source=source):
            for target, g in order(source):
                line_copy(source, target, g).start()

    w_copy.wait()
    bias_copy.wait()
    bias = bias_ref[...]
    w_hi, w_lo = split(w_ref[...], 2)
    b_hi, b_mid, b_lo = [part.astype(F32) for part in split(bias, 3)]
    at = lax.broadcasted_iota(I32, (16, width), 0)
    extra = jnp.where(at == 0, b_hi, jnp.where(at == 1, b_mid, jnp.where(at == 2, b_lo, 0.0)))
    wcat[...] = jnp.concatenate([w_hi, w_lo, w_hi, extra.astype(BF16)], 0)

    lane = lax.broadcasted_iota(I32, (GROUP, height), 1)

    def bound(index):
        return wide(jnp.broadcast_to(prefix[index], (GROUP, 128)), height)

    def turn(ref, slot, index, g):
        shift = (prefix[index] & (height - 1))[0, 0]
        return pltpu.roll(ref[slot, g * GROUP : (g + 1) * GROUP], shift, 1)

    def routed(z):
        base = seat * height + lane
        told(side - 1, count_recv.at[0])
        for target in range(z):
            if not far(z, target):
                line_count(z, target).start()
        if z == 1:
            told(side, line_recv.at[0])
        for target in range(z + 1, lines):
            if tells(z, target):
                line_count(z, target).start()
        if z > 1:
            told(2 * side, line_recv.at[1])
            for source in range(2, z):
                told(side, line_recv.at[source])
        extend(0, (z + 1) * side)
        low, high = bound(z * side), bound(z * side + side)
        relayed = z == 3
        merges = z == 2 and lines > 3
        for g in range(groups):
            at_g = slice(g * GROUP, (g + 1) * GROUP)
            arrived(side - 1, g, gather_recv.at[g])
            blocks = [turn(gather, at, z * side + at, g) for at in range(side)]

            def choose(place):
                piece = jnp.where(place >= low, blocks[0], 0.0)
                for at in range(1, side):
                    piece = jnp.where(place >= bound(z * side + at), blocks[at], piece)
                return jnp.where(place >= high, 0.0, piece)

            if relayed:
                mixed = choose(low + ((base - low) & (side * height - 1)))
                pieces[2, at_g] = mixed
                down_copy(3, 2, g).start()
                joined[1, at_g] = jnp.where(z * side * height + base < low + side * height, mixed, 0.0)
            else:
                for target in range(z):
                    pieces[target, at_g] = choose(target * side * height + base)
                    if not merges:
                        down_copy(z, target, g).start()
                joined[1, at_g] = choose(z * side * height + base)
            if relayed:
                join_copy(1, g).start()
        for source in range(z + 1, lines):
            if not far(source, z):
                told(side, line_recv.at[source])
        if z == 0 and lines > 2:
            told((lines - 2) * side, count_recv.at[2])
        extend((z + 1) * side, n)
        total_copy().start()
        def merge():
            for g in range(groups):
                at_g = slice(g * GROUP, (g + 1) * GROUP)
                arrived(1, g, piece_recv.at[g])
                for target in range(3):
                    place = target * side * height + base
                    inside = jnp.logical_and(place >= high, place < high + side * height)
                    block = jnp.where(inside, got[3, at_g], joined[1, at_g] if target == 2 else pieces[target, at_g])
                    if target == 2:
                        joined[1, at_g] = block
                        join_copy(1, g).start()
                    else:
                        pieces[target, at_g] = block
                        if target == 0:
                            down_copy(2, 0, g).start()
            for g in range(groups):
                down_copy(2, 1, g).start()

        sources = range(z, lines)
        for g in range(groups):
            if merges and g == MERGE:
                merge()
            at_g = slice(g * GROUP, (g + 1) * GROUP)
            arrived(lines - z, g, heap_recv.at[g])
            turned = [turn(heap, at, at * side + seat, g) for at in sources]
            for step in [*range(1, side), 0]:
                place = (z * side + flip(seat, step, side)) * height + lane
                piece = jnp.zeros((GROUP, height), F32)
                for at, block in zip(sources, turned):
                    index = at * side + seat
                    inside = jnp.logical_and(place >= bound(index), place < bound(index + 1))
                    piece = jnp.where(inside, block, piece)
                if step:
                    parts[step, at_g] = piece
                    across_copy(step, g).start()
                else:
                    joined[0, at_g] = piece
        def take_flat(g):
            froms = range(z + 1, min(lines, 3))
            at_g = slice(g * GROUP, (g + 1) * GROUP)
            if froms:
                arrived(len(froms), g, piece_recv.at[g])
                block = joined[1, at_g]
                for source in froms:
                    block = block + got[source, at_g]
                joined[1, at_g] = block
            join_copy(1, g).start()

        def take_tall(g):
            at_g = slice(g * GROUP, (g + 1) * GROUP)
            arrived(side - 1, g, across_recv.at[g])
            block = joined[0, at_g]
            for step in range(1, side):
                block = block + came[step, at_g]
            joined[0, at_g] = block
            join_copy(0, g).start()

        for g in range(groups):
            take_tall(g)
            if not merges and not relayed:
                take_flat(g)

    for z in range(lines):
        @pl.when(jnp.logical_and(flat, line == z))
        def _(z=z):
            routed(z)

    @pl.when(core == 0)
    def _():
        at = prefix.at[n]
        remote(at, at, count_send.at[3], count_recv.at[1], section=1 - core).wait_recv()
        remote(joined, joined, join_send.at[0], join_recv.at[0], section=1 - core).wait_recv()

    ends = wide(prefix[n], lanes)
    for chunk in range(CHUNKS):
        at = slice(chunk * lanes, (chunk + 1) * lanes)
        owned = me * height + chunk * lanes + lax.broadcasted_iota(I32, (1, lanes), 1)
        filled = jnp.where(owned < ends, 1.0, 0.0)
        block = jnp.concatenate([joined[0, :, at], joined[1, :, at]], 0)
        a_hi, a_lo = split(block, 2)
        marks = jnp.broadcast_to(filled, (16, lanes)).astype(BF16)
        lhs = jnp.concatenate([a_hi, a_hi, a_lo, marks], 0)
        out_ref[at, :] = lax.dot_general(
            lhs, wcat[...], (((0,), (0,)), ((), ())), preferred_element_type=F32
        ).astype(BF16)

    for z in range(lines):
        @pl.when(jnp.logical_and(flat, line == z))
        def _(z=z):
            said(side - 1, count_send.at[0])
            below = sum(not far(z, target) for target in range(z))
            if below:
                said(below * side, count_send.at[1])
            above = sum(tells(z, target) for target in range(z + 1, lines))
            if above:
                said(above * side * (2 if z == 1 else 1), count_send.at[2])
            total_copy().wait_send()
            left(side - 1, gather_send.at[0])
            if z:
                left(1 if z == 3 else z, piece_send.at[0])
            left(side - 1, across_send.at[0])
            left(2, join_send.at[0])

        @pl.when(jnp.logical_and(core == 0, line == z))
        def _(z=z):
            left(z + 1, gather_send.at[0])
            if z > 1:
                said(side, count_send.at[1])


def solution(mesh):
    n, sections = mesh.shape["rows"], mesh.shape["section"]

    def step(table, mask, weight, bias):
        height, half = table.shape
        cols, features = weight.shape
        width = features // sections
        levels = (n - 1).bit_length()
        side, crowd = min(PLANE, n), min(RAW, n)
        lines, groups = n // side, half // GROUP
        operands = table.T, mask.reshape(height // 128, 128), weight, bias.reshape(1, features)
        sem = pltpu.SemaphoreType.DMA
        loads = [
            pltpu.VMEM((half, height), F32),
            pltpu.VMEM((height // 128, 128), I32),
            pltpu.VMEM((1, width), F32),
        ]
        weights = [
            pltpu.VMEM((cols, width), F32),
            pltpu.VMEM((3 * cols + 16, width), BF16),
        ]
        if lines <= LINES:
            most = max(side, lines)
            block = pltpu.VMEM((most, half, height), F32)
            body = direct
            scratch = loads + [
                pltpu.VMEM((n, 1, 128), I32),
                pltpu.VMEM((n + 1, 1, 128), I32),
                block, block, block, block, block, block,
                pltpu.VMEM((sections, half, height), F32),
            ] + weights + [
                sem((4,)), sem((4,)), sem((3,)), sem((lines,)),
                sem((1,)), sem((groups,)), sem((groups,)),
                sem((1,)), sem((groups,)), sem((1,)), sem((groups,)),
                sem((1,)), sem((1,)),
            ]
        else:
            body = butterfly
            scratch = loads + [
                pltpu.VMEM((side, 1, 128), I32),
                pltpu.VMEM((n // side, 1, 128), I32),
                pltpu.VMEM((n + 1, 1, 128), I32),
                pltpu.VMEM((crowd, half, height), F32),
                pltpu.VMEM((levels, half, height), F32),
                pltpu.VMEM((levels, half, height), F32),
                pltpu.VMEM((sections, half, height), F32),
            ] + weights + [
                sem((levels + 1, CHUNKS)), sem((levels + 1, CHUNKS)),
                sem((crowd,)), sem((crowd,)),
                sem((side,)), sem((side,)),
                sem((n // side,)), sem((n // side,)),
                sem((4,)),
            ]
        return pl.pallas_call(
            functools.partial(body, n),
            name="filter_project",
            out_shape=jax.ShapeDtypeStruct((height, width), BF16),
            in_specs=[pl.BlockSpec(memory_space=pltpu.HBM)] * 4,
            out_specs=pl.BlockSpec(memory_space=pltpu.VMEM),
            scratch_shapes=scratch,
            compiler_params=pltpu.CompilerParams(
                collective_id=0, has_side_effects=True, vmem_limit_bytes=16 << 20
            ),
        )(*[pltpu.with_memory_space_constraint(x, pltpu.HBM) for x in operands])

    return jax.shard_map(
        step,
        mesh=mesh,
        in_specs=(P("rows", "section"), P("rows"), P(), P()),
        out_specs=P("rows", "section"),
        check_vma=False,
    )
```

```python
import functools

import jax
import jax.numpy as jnp
from jax import lax
from jax.experimental import pallas as pl
from jax.experimental.pallas import tpu as pltpu
from jax.sharding import PartitionSpec as P

CHUNKS = 4
PLANE = 4
RAW = 4
LINES = 4
GROUP = 8
TERMS = 2
MERGE = 2
EARLY = 4
F32 = jnp.float32
BF16 = jnp.bfloat16
I32 = jnp.int32


def split(x, terms):
    parts = []
    for _ in range(terms):
        part = x.astype(BF16)
        parts.append(part)
        x = x - part.astype(F32)
    return parts


def butterfly(
    n, table_hbm, mask_hbm, w_hbm, bias_hbm, out_ref,
    table_ref, mask_ref, bias_ref,
    tally, planes, prefix, raw, hold, came, joined, w_ref, wcat,
    send_sem, recv_sem, raw_send, raw_recv, count_send, count_recv, plane_send, plane_recv, load_sem,
):
    half, height = table_hbm.shape
    width = out_ref.shape[1]
    lines = height // 128
    levels = (n - 1).bit_length()
    lanes = height // CHUNKS
    side = min(PLANE, n)
    crowd = min(RAW, n)
    first = (crowd - 1).bit_length()
    count_planes = n // side
    me = lax.axis_index("rows")
    core = lax.axis_index("section")
    plane = me // side
    seat = lax.rem(me, side)

    columns = pl.ds(pl.multiple_of(core * width, 128), width)
    mask_copy = pltpu.make_async_copy(mask_hbm, mask_ref, load_sem.at[0])
    table_copy = pltpu.make_async_copy(table_hbm, table_ref, load_sem.at[1])
    w_copy = pltpu.make_async_copy(w_hbm.at[:, columns], w_ref, load_sem.at[2])
    bias_copy = pltpu.make_async_copy(bias_hbm.at[:, columns], bias_ref, load_sem.at[3])
    for load in (mask_copy, table_copy, w_copy, bias_copy):
        load.start()

    def seat_peer(step):
        return plane * side + lax.rem(seat + step, side)

    def plane_peer(step):
        return lax.rem(plane + step, count_planes) * side + seat

    barrier = pltpu.get_barrier_semaphore()
    for step in range(1, side):
        pl.semaphore_signal(barrier, inc=1, device_id={"rows": seat_peer(step)})
    for step in range(1, count_planes):
        pl.semaphore_signal(barrier, inc=1, device_id={"rows": plane_peer(step)})
    pl.semaphore_signal(barrier, inc=1, device_id={"section": 1 - core})

    mask_copy.wait()
    mask = mask_ref[...]
    ones = mask.astype(F32).astype(BF16)
    row = lax.broadcasted_iota(I32, (128, 128), 0)
    col = lax.broadcasted_iota(I32, (128, 128), 1)
    before = jnp.where(row < col, 1.0, 0.0).astype(BF16)
    inner = jnp.dot(ones, before, preferred_element_type=F32).astype(I32)
    sums = jnp.dot(ones, jnp.ones((128, 128), BF16), preferred_element_type=F32).astype(I32)
    running = jnp.zeros((1, 128), I32)
    starts = []
    for line in range(lines):
        starts.append(running)
        running = running + sums[line : line + 1]
    tally[seat] = running
    slot = jnp.where(mask == 1, inner + jnp.concatenate(starts, 0), -1)

    own = lax.rem(me, crowd)
    table_copy.wait()
    turned = jnp.concatenate(split(table_ref[...], 3), 0)
    for chunk in range(CHUNKS):
        here = chunk * lanes + lax.broadcasted_iota(I32, (lanes, 128), 0)
        hot = jnp.concatenate(
            [jnp.where(here == slot[b : b + 1], 1.0, 0.0).astype(BF16) for b in range(chunk * lanes // 128, lines)], 1
        )
        folded = lax.dot_general(
            turned[:, chunk * lanes :], hot, (((1,), (1,)), ((), ())), preferred_element_type=F32
        )
        raw[own, :, chunk * lanes : (chunk + 1) * lanes] = (
            folded[:half] + folded[half : 2 * half]
        ) + folded[2 * half :]

    pl.semaphore_wait(barrier, side + count_planes - 1)

    def seat_copy(step):
        return pltpu.make_async_remote_copy(
            src_ref=tally.at[seat], dst_ref=tally.at[seat],
            send_sem=count_send.at[step], recv_sem=count_recv.at[step],
            device_id={"rows": seat_peer(step)},
        )

    def plane_copy(step):
        return pltpu.make_async_remote_copy(
            src_ref=planes.at[plane], dst_ref=planes.at[plane],
            send_sem=plane_send.at[step], recv_sem=plane_recv.at[step],
            device_id={"rows": plane_peer(step)},
        )

    def raw_copy(step):
        return pltpu.make_async_remote_copy(
            src_ref=raw.at[own], dst_ref=raw.at[own],
            send_sem=raw_send.at[step], recv_sem=raw_recv.at[step],
            device_id={"rows": me - own + lax.rem(own + step, crowd)},
        )

    for step in range(1, side):
        seat_copy(step).start()
    for step in range(1, crowd):
        raw_copy(step).start()
    for step in range(1, side):
        seat_copy(step).wait_recv()
    everyone = jnp.zeros((1, 128), I32)
    for at in range(side):
        everyone = everyone + tally[at]
    planes[plane] = everyone
    for step in range(1, count_planes):
        plane_copy(step).start()

    w_copy.wait()
    bias_copy.wait()
    bias = bias_ref[...]
    w_hi, w_lo = split(w_ref[...], 2)
    b_hi, b_mid, b_lo = [part.astype(F32) for part in split(bias, 3)]
    line = lax.broadcasted_iota(I32, (16, width), 0)
    extra = jnp.where(line == 0, b_hi, jnp.where(line == 1, b_mid, jnp.where(line == 2, b_lo, 0.0)))
    wcat[...] = jnp.concatenate([w_hi, w_lo, w_hi, extra.astype(BF16)], 0)

    for step in range(1, count_planes):
        plane_copy(step).wait_recv()
    total = jnp.zeros((1, 128), I32)
    for at in range(count_planes):
        prefix[at * side] = total
        total = total + planes[at]
    prefix[n] = total
    running = prefix[plane * side]
    for at in range(side - 1):
        running = running + tally[at]
        prefix[plane * side + at + 1] = running

    def wide(x):
        return jnp.concatenate([x] * (lanes // 128), 1)

    def data_copy(level, chunk):
        at = (slice(None), pl.ds(chunk * lanes, lanes))
        return pltpu.make_async_remote_copy(
            src_ref=hold.at[(level,) + at], dst_ref=came.at[(level,) + at],
            send_sem=send_sem.at[level, chunk], recv_sem=recv_sem.at[level, chunk],
            device_id={"rows": me + (1 - 2 * (me // (1 << level) % 2)) * (1 << level)},
        )

    def join_copy(chunk):
        at = (core, slice(None), pl.ds(chunk * lanes, lanes))
        return pltpu.make_async_remote_copy(
            src_ref=joined.at[at], dst_ref=joined.at[at],
            send_sem=send_sem.at[levels, chunk], recv_sem=recv_sem.at[levels, chunk],
            device_id={"section": 1 - core},
        )

    for step in range(1, crowd):
        raw_copy(step).wait_recv()
    turns = []
    for at in range(crowd):
        shift = (prefix[me - own + at] & (height - 1))[0, 0]
        turns.append(pltpu.roll(raw[at], shift, 1))
    low = wide(prefix[me - own])
    for chunk in range(CHUNKS):
        at = slice(chunk * lanes, (chunk + 1) * lanes)
        base = own * height + chunk * lanes + lax.broadcasted_iota(I32, (1, lanes), 1)
        place = low + ((base - low) & (crowd * height - 1))
        place = jnp.broadcast_to(place, (half, lanes))
        block = turns[0][:, at]
        for other in range(1, crowd):
            block = jnp.where(place >= wide(prefix[me - own + other]), turns[other][:, at], block)
        hold[first, :, at] = block
        data_copy(first, chunk).start()

    for level in range(first, levels):
        reach = 2 << level
        group = me // reach * reach
        bit = me // (1 << level) % 2
        low = wide(prefix[group])
        middle = wide(prefix[group + (1 << level)])
        for chunk in range(CHUNKS):
            at = slice(chunk * lanes, (chunk + 1) * lanes)
            data_copy(level, chunk).wait_recv()
            base = (me % reach) * height + chunk * lanes
            base = base + lax.broadcasted_iota(I32, (1, lanes), 1)
            place = low + ((base - low) & (reach * height - 1))
            upper = jnp.where(place >= middle, 1, 0)
            foreign = jnp.broadcast_to(upper, (half, lanes)) != bit
            block = jnp.where(foreign, came[level, :, at], hold[level, :, at])
            if level < levels - 1:
                hold[level + 1, :, at] = block
                data_copy(level + 1, chunk).start()
            else:
                joined[core, :, at] = block
                join_copy(chunk).start()

    ends = wide(total)
    for chunk in range(CHUNKS):
        at = slice(chunk * lanes, (chunk + 1) * lanes)
        join_copy(chunk).wait_recv()
        owned = me * height + chunk * lanes + lax.broadcasted_iota(I32, (1, lanes), 1)
        filled = jnp.where(owned < ends, 1.0, 0.0)
        rows = jnp.concatenate([joined[0, :, at], joined[1, :, at]], 0)
        rows = jnp.where(jnp.broadcast_to(filled, rows.shape) > 0.5, rows, 0.0)
        a_hi, a_lo = split(rows, 2)
        marks = jnp.broadcast_to(filled, (16, lanes)).astype(BF16)
        lhs = jnp.concatenate([a_hi, a_hi, a_lo, marks], 0)
        out_ref[at, :] = lax.dot_general(
            lhs, wcat[...], (((0,), (0,)), ((), ())), preferred_element_type=F32
        ).astype(BF16)

    for step in range(1, side):
        seat_copy(step).wait_send()
    for step in range(1, count_planes):
        plane_copy(step).wait_send()
    for step in range(1, crowd):
        raw_copy(step).wait_send()
    for level in range(first, levels):
        for chunk in range(CHUNKS):
            data_copy(level, chunk).wait_send()
    for chunk in range(CHUNKS):
        join_copy(chunk).wait_send()


def wide(x, lanes):
    return jnp.concatenate([x] * (lanes // 128), 1)


def flip(at, step, extent):
    out, bit = 0, 1
    while bit < extent:
        a, b = at // bit % 2, step // bit % 2
        out = out + bit * (a + b - 2 * a * b)
        bit *= 2
    return out


def direct(
    n, table_hbm, mask_hbm, w_hbm, bias_hbm, out_ref,
    table_ref, mask_ref, bias_ref,
    tally, prefix, gather, heap, pieces, parts, got, came, joined, w_ref, wcat,
    load_sem, count_send, count_recv, line_recv, gather_send, gather_recv, heap_recv,
    piece_send, piece_recv, across_send, across_recv, join_send, join_recv, ready,
):
    half, height = table_hbm.shape
    width = out_ref.shape[1]
    rows = height // 128
    lanes = height // CHUNKS
    groups = half // GROUP
    side = min(PLANE, n)
    lines = n // side
    me = lax.axis_index("rows")
    core = lax.axis_index("section")
    line = me // side
    seat = lax.rem(me, side)
    flat = core == 1

    columns = pl.ds(pl.multiple_of(core * width, 128), width)
    mask_copy = pltpu.make_async_copy(mask_hbm, mask_ref, load_sem.at[0])
    table_copy = pltpu.make_async_copy(table_hbm, table_ref, load_sem.at[1])
    w_copy = pltpu.make_async_copy(w_hbm.at[:, columns], w_ref, load_sem.at[2])
    bias_copy = pltpu.make_async_copy(bias_hbm.at[:, columns], bias_ref, load_sem.at[3])
    for load in (mask_copy, table_copy, w_copy, bias_copy):
        load.start()

    barrier = pltpu.get_barrier_semaphore()
    pl.semaphore_signal(barrier, inc=1, device_id={"section": 1 - core})

    def tells(source, target):
        return source != target and not (source == 0 and target > 1)

    def later(source, target):
        return source < 2 and target > source

    def far(source, target):
        return source > 1 and target == 0

    @pl.when(flat)
    def _():
        for step in range(1, side):
            pl.semaphore_signal(barrier, inc=1, device_id={"rows": line * side + flip(seat, step, side)})
        for other in range(lines):
            for z in range(lines):
                if tells(other, z) and not later(other, z):
                    @pl.when(line == z)
                    def _(other=other):
                        pl.semaphore_signal(barrier, inc=1, device_id={"rows": other * side + seat})
            for z in range(other):
                @pl.when(line == z)
                def _(other=other, z=z):
                    for at in range(side) if far(other, z) else [seat]:
                        pl.semaphore_signal(barrier, inc=1, device_id={"rows": other * side + at, "section": 0})

    mask_copy.wait()
    mask = mask_ref[...]
    ones = mask.astype(F32).astype(BF16)
    row = lax.broadcasted_iota(I32, (128, 128), 0)
    col = lax.broadcasted_iota(I32, (128, 128), 1)
    before = jnp.where(row < col, 1.0, 0.0).astype(BF16)
    inner = jnp.dot(ones, before, preferred_element_type=F32).astype(I32)
    sums = jnp.dot(ones, jnp.ones((128, 128), BF16), preferred_element_type=F32).astype(I32)
    running = jnp.zeros((1, 128), I32)
    starts = []
    for at in range(rows):
        starts.append(running)
        running = running + sums[at : at + 1]
    tally[me] = running
    slot = jnp.where(mask == 1, inner + jnp.concatenate(starts, 0), -1)

    def far_count():
        at = tally.at[me]
        return [
            pltpu.make_async_remote_copy(
                src_ref=at, dst_ref=at, send_sem=count_send.at[1], recv_sem=count_recv.at[2],
                device_id={"rows": to, "section": 1},
            )
            for to in range(side)
        ]

    for z in range(lines):
        @pl.when(jnp.logical_and(core == 0, line == z))
        def _(z=z):
            pl.semaphore_wait(barrier, 1 + z + (side - 1 if z > 1 else 0))
            if z > 1:
                for copy in far_count():
                    copy.start()

    def seat_count():
        at = tally.at[me]
        return [
            pltpu.make_async_remote_copy(
                src_ref=at, dst_ref=at, send_sem=count_send.at[0], recv_sem=count_recv.at[0],
                device_id={"rows": line * side + flip(seat, step, side)},
            )
            for step in range(1, side)
        ]

    def enter(z):
        ahead = sum(tells(z, other) and not later(z, other) for other in range(lines))
        pl.semaphore_wait(barrier, side + ahead)
        for other in range(min(z, 2)):
            if tells(other, z):
                pl.semaphore_signal(ready, inc=1, device_id={"rows": other * side + seat})
        for copy in seat_count():
            copy.start()

    for z in range(min(lines, 2)):
        @pl.when(jnp.logical_and(flat, line == z))
        def _(z=z):
            enter(z)

    own = jnp.where(flat, seat, line)
    table_copy.wait()
    terms = jnp.concatenate(split(table_ref[...], TERMS), 0)
    for chunk in range(CHUNKS):
        here = chunk * lanes + lax.broadcasted_iota(I32, (lanes, 128), 0)
        hot = jnp.concatenate(
            [jnp.where(here == slot[b : b + 1], 1.0, 0.0).astype(BF16) for b in range(chunk * lanes // 128, rows)], 1
        )
        folded = lax.dot_general(
            terms[:, chunk * lanes :], hot, (((1,), (1,)), ((), ())), preferred_element_type=F32
        )
        block = folded[:half]
        for term in range(1, TERMS):
            block = block + folded[term * half : (term + 1) * half]
        gather[own, :, chunk * lanes : (chunk + 1) * lanes] = block

    def span(g):
        return pl.ds(g * GROUP, GROUP)

    def remote(src, dst, send, recv, **to):
        return pltpu.make_async_remote_copy(src_ref=src, dst_ref=dst, send_sem=send, recv_sem=recv, device_id=to)

    def line_count(source, target):
        low = 0 if target > source == 1 else source * side
        at = tally.at[pl.ds(low, (source + 1) * side - low)]
        return remote(
            at, at, count_send.at[2 if target > source else 1], line_recv.at[source], rows=target * side + seat
        )

    def total_copy():
        at = prefix.at[n]
        return remote(at, at, count_send.at[3], count_recv.at[1], section=1 - core)

    def seat_copy(step, g):
        at = gather.at[seat, span(g)]
        to = line * side + flip(seat, step, side)
        return remote(at, at, gather_send.at[0], gather_recv.at[g], rows=to)

    def line_copy(source, target, g):
        return remote(
            gather.at[source, span(g)], heap.at[source, span(g)],
            gather_send.at[0], heap_recv.at[g], rows=target * side + seat, section=1,
        )

    def order(source):
        every = range(groups)
        first = [(0, g) for g in every] if source else []
        near = [(target, g) for target in reversed(range(2, source)) for g in every]
        after = [(source, g) for g in every] + [(1, g) for g in every if source == 2]
        return first[:EARLY] + near + first[EARLY:] + after

    def pass_copy(g):
        at = heap.at[3, span(g)]
        return remote(at, at, gather_send.at[0], heap_recv.at[g], rows=side + seat)

    def down_copy(source, target, g):
        return remote(
            pieces.at[target, span(g)], got.at[source, span(g)],
            piece_send.at[0], piece_recv.at[g], rows=target * side + seat,
        )

    def across_copy(step, g):
        return remote(
            parts.at[step, span(g)], came.at[step, span(g)],
            across_send.at[0], across_recv.at[g], rows=line * side + flip(seat, step, side),
        )

    def join_copy(which, g):
        at = joined.at[which, span(g)]
        return remote(at, at, join_send.at[0], join_recv.at[0], section=1 - core)

    def arrived(count, g, sem):
        at = heap.at[pl.ds(0, count), span(g)]
        remote(at, at, sem, sem, section=core).wait_recv()

    def left(count, sem):
        at = heap.at[pl.ds(0, count)]
        remote(at, at, sem, sem, section=core).wait_send()

    def told(count, sem):
        at = tally.at[pl.ds(0, count)]
        remote(at, at, sem, sem, section=core).wait_recv()

    def said(count, sem):
        at = tally.at[pl.ds(0, count)]
        remote(at, at, sem, sem, section=core).wait_send()

    def extend(start, stop):
        running = prefix[start] if start else jnp.zeros((1, 128), I32)
        prefix[start] = running
        for at in range(start, stop):
            running = running + tally[at]
            prefix[at + 1] = running

    for z in range(2, lines):
        @pl.when(jnp.logical_and(flat, line == z))
        def _(z=z):
            enter(z)

    @pl.when(flat)
    def _():
        for g in range(groups):
            for step in range(1, side):
                seat_copy(step, g).start()

    for source in range(lines):
        @pl.when(jnp.logical_and(core == 0, line == source))
        def _(source=source):
            for target, g in order(source):
                line_copy(source, target, g).start()

    w_copy.wait()
    bias_copy.wait()
    bias = bias_ref[...]
    w_hi, w_lo = split(w_ref[...], 2)
    b_hi, b_mid, b_lo = [part.astype(F32) for part in split(bias, 3)]
    at = lax.broadcasted_iota(I32, (16, width), 0)
    extra = jnp.where(at == 0, b_hi, jnp.where(at == 1, b_mid, jnp.where(at == 2, b_lo, 0.0)))
    wcat[...] = jnp.concatenate([w_hi, w_lo, w_hi, extra.astype(BF16)], 0)

    lane = lax.broadcasted_iota(I32, (GROUP, height), 1)

    def bound(index):
        return wide(jnp.broadcast_to(prefix[index], (GROUP, 128)), height)

    def turn(ref, slot, index, g):
        shift = (prefix[index] & (height - 1))[0, 0]
        return pltpu.roll(ref[slot, g * GROUP : (g + 1) * GROUP], shift, 1)

    def routed(z):
        base = seat * height + lane
        told(side - 1, count_recv.at[0])
        for target in range(z):
            if not far(z, target):
                line_count(z, target).start()
        if z == 1:
            told(side, line_recv.at[0])
        above = [target for target in range(z + 1, lines) if tells(z, target)]
        if z < 2 and above:
            pl.semaphore_wait(ready, len(above))
        for target in above:
            line_count(z, target).start()
        if z > 1:
            told(2 * side, line_recv.at[1])
            for source in range(2, z):
                told(side, line_recv.at[source])
        extend(0, (z + 1) * side)
        low, high = bound(z * side), bound(z * side + side)
        relayed = z == 3
        merges = z == 2 and lines > 3
        if merges:
            for g in range(groups):
                arrived(lines - z, g, heap_recv.at[g])
                pass_copy(g).start()
        for g in range(groups):
            at_g = slice(g * GROUP, (g + 1) * GROUP)
            arrived(side - 1, g, gather_recv.at[g])
            blocks = [turn(gather, at, z * side + at, g) for at in range(side)]

            def choose(place):
                piece = jnp.where(place >= low, blocks[0], 0.0)
                for at in range(1, side):
                    piece = jnp.where(place >= bound(z * side + at), blocks[at], piece)
                return jnp.where(place >= high, 0.0, piece)

            if relayed:
                mixed = choose(low + ((base - low) & (side * height - 1)))
                pieces[2, at_g] = mixed
                down_copy(3, 2, g).start()
                joined[1, at_g] = jnp.where(z * side * height + base < low + side * height, mixed, 0.0)
            else:
                for target in range(z):
                    pieces[target, at_g] = choose(target * side * height + base)
                    if not merges:
                        down_copy(z, target, g).start()
                joined[1, at_g] = choose(z * side * height + base)
            if relayed:
                join_copy(1, g).start()
        for source in range(z + 1, lines):
            if not far(source, z):
                told(side, line_recv.at[source])
        if z == 0 and lines > 2:
            told((lines - 2) * side, count_recv.at[2])
        extend((z + 1) * side, n)
        total_copy().start()
        def merge():
            for g in range(groups):
                at_g = slice(g * GROUP, (g + 1) * GROUP)
                arrived(1, g, piece_recv.at[g])
                for target in range(3):
                    place = target * side * height + base
                    inside = jnp.logical_and(place >= high, place < high + side * height)
                    block = jnp.where(inside, got[3, at_g], joined[1, at_g] if target == 2 else pieces[target, at_g])
                    if target == 2:
                        joined[1, at_g] = block
                        join_copy(1, g).start()
                    else:
                        pieces[target, at_g] = block
                        if target == 0:
                            down_copy(2, 0, g).start()
            for g in range(groups):
                down_copy(2, 1, g).start()

        sources = range(z, lines)
        for g in range(groups):
            if merges and g == MERGE:
                merge()
            at_g = slice(g * GROUP, (g + 1) * GROUP)
            if not merges:
                arrived(lines - z, g, heap_recv.at[g])
            turned = [turn(heap, at, at * side + seat, g) for at in sources]
            for step in [*range(1, side), 0]:
                place = (z * side + flip(seat, step, side)) * height + lane
                piece = jnp.zeros((GROUP, height), F32)
                for at, block in zip(sources, turned):
                    index = at * side + seat
                    inside = jnp.logical_and(place >= bound(index), place < bound(index + 1))
                    piece = jnp.where(inside, block, piece)
                if step:
                    parts[step, at_g] = piece
                    across_copy(step, g).start()
                else:
                    joined[0, at_g] = piece
        def take_flat(g):
            froms = range(z + 1, min(lines, 3))
            at_g = slice(g * GROUP, (g + 1) * GROUP)
            if froms:
                arrived(len(froms), g, piece_recv.at[g])
                block = joined[1, at_g]
                for source in froms:
                    block = block + got[source, at_g]
                joined[1, at_g] = block
            join_copy(1, g).start()

        def take_tall(g):
            at_g = slice(g * GROUP, (g + 1) * GROUP)
            arrived(side - 1, g, across_recv.at[g])
            block = joined[0, at_g]
            for step in range(1, side):
                block = block + came[step, at_g]
            joined[0, at_g] = block
            join_copy(0, g).start()

        for g in range(groups):
            take_tall(g)
            if not merges and not relayed:
                take_flat(g)

    for z in range(lines):
        @pl.when(jnp.logical_and(flat, line == z))
        def _(z=z):
            routed(z)

    @pl.when(core == 0)
    def _():
        at = prefix.at[n]
        remote(at, at, count_send.at[3], count_recv.at[1], section=1 - core).wait_recv()
        remote(joined, joined, join_send.at[0], join_recv.at[0], section=1 - core).wait_recv()

    ends = wide(prefix[n], lanes)
    for chunk in range(CHUNKS):
        at = slice(chunk * lanes, (chunk + 1) * lanes)
        owned = me * height + chunk * lanes + lax.broadcasted_iota(I32, (1, lanes), 1)
        filled = jnp.where(owned < ends, 1.0, 0.0)
        block = jnp.concatenate([joined[0, :, at], joined[1, :, at]], 0)
        a_hi, a_lo = split(block, 2)
        marks = jnp.broadcast_to(filled, (16, lanes)).astype(BF16)
        lhs = jnp.concatenate([a_hi, a_hi, a_lo, marks], 0)
        out_ref[at, :] = lax.dot_general(
            lhs, wcat[...], (((0,), (0,)), ((), ())), preferred_element_type=F32
        ).astype(BF16)

    for z in range(lines):
        @pl.when(jnp.logical_and(flat, line == z))
        def _(z=z):
            said(side - 1, count_send.at[0])
            below = sum(not far(z, target) for target in range(z))
            if below:
                said(below * side, count_send.at[1])
            above = sum(tells(z, target) for target in range(z + 1, lines))
            if above:
                said(above * side * (2 if z == 1 else 1), count_send.at[2])
            total_copy().wait_send()
            left(side - 1, gather_send.at[0])
            if z == 2 and lines > 3:
                left(1, gather_send.at[0])
            if z:
                left(1 if z == 3 else z, piece_send.at[0])
            left(side - 1, across_send.at[0])
            left(2, join_send.at[0])

        @pl.when(jnp.logical_and(core == 0, line == z))
        def _(z=z):
            left(min(z + 1, 3), gather_send.at[0])
            if z > 1:
                said(side, count_send.at[1])


def solution(mesh):
    n, sections = mesh.shape["rows"], mesh.shape["section"]

    def step(table, mask, weight, bias):
        height, half = table.shape
        cols, features = weight.shape
        width = features // sections
        levels = (n - 1).bit_length()
        side, crowd = min(PLANE, n), min(RAW, n)
        lines, groups = n // side, half // GROUP
        operands = table.T, mask.reshape(height // 128, 128), weight, bias.reshape(1, features)
        sem = pltpu.SemaphoreType.DMA
        loads = [
            pltpu.VMEM((half, height), F32),
            pltpu.VMEM((height // 128, 128), I32),
            pltpu.VMEM((1, width), F32),
        ]
        weights = [
            pltpu.VMEM((cols, width), F32),
            pltpu.VMEM((3 * cols + 16, width), BF16),
        ]
        if lines <= LINES:
            most = max(side, lines)
            block = pltpu.VMEM((most, half, height), F32)
            body = direct
            scratch = loads + [
                pltpu.VMEM((n, 1, 128), I32),
                pltpu.VMEM((n + 1, 1, 128), I32),
                block, block, block, block, block, block,
                pltpu.VMEM((sections, half, height), F32),
            ] + weights + [
                sem((4,)), sem((4,)), sem((3,)), sem((lines,)),
                sem((1,)), sem((groups,)), sem((groups,)),
                sem((1,)), sem((groups,)), sem((1,)), sem((groups,)),
                sem((1,)), sem((1,)), pltpu.SemaphoreType.REGULAR,
            ]
        else:
            body = butterfly
            scratch = loads + [
                pltpu.VMEM((side, 1, 128), I32),
                pltpu.VMEM((n // side, 1, 128), I32),
                pltpu.VMEM((n + 1, 1, 128), I32),
                pltpu.VMEM((crowd, half, height), F32),
                pltpu.VMEM((levels, half, height), F32),
                pltpu.VMEM((levels, half, height), F32),
                pltpu.VMEM((sections, half, height), F32),
            ] + weights + [
                sem((levels + 1, CHUNKS)), sem((levels + 1, CHUNKS)),
                sem((crowd,)), sem((crowd,)),
                sem((side,)), sem((side,)),
                sem((n // side,)), sem((n // side,)),
                sem((4,)),
            ]
        return pl.pallas_call(
            functools.partial(body, n),
            name="filter_project",
            out_shape=jax.ShapeDtypeStruct((height, width), BF16),
            in_specs=[pl.BlockSpec(memory_space=pltpu.HBM)] * 4,
            out_specs=pl.BlockSpec(memory_space=pltpu.VMEM),
            scratch_shapes=scratch,
            compiler_params=pltpu.CompilerParams(
                collective_id=0, has_side_effects=True, vmem_limit_bytes=16 << 20
            ),
        )(*[pltpu.with_memory_space_constraint(x, pltpu.HBM) for x in operands])

    return jax.shard_map(
        step,
        mesh=mesh,
        in_specs=(P("rows", "section"), P("rows"), P(), P()),
        out_specs=P("rows", "section"),
        check_vma=False,
    )
```

```python
import functools

import jax
import jax.numpy as jnp
from jax import lax
from jax.experimental import pallas as pl
from jax.experimental.pallas import tpu as pltpu
from jax.sharding import PartitionSpec as P

CHUNKS = 4
PLANE = 4
RAW = 4
LINES = 4
GROUP = 8
TERMS = 2
MERGE = 1
EARLY = 3
LIFT = 1
F32 = jnp.float32
BF16 = jnp.bfloat16
I32 = jnp.int32


def split(x, terms):
    parts = []
    for _ in range(terms):
        part = x.astype(BF16)
        parts.append(part)
        x = x - part.astype(F32)
    return parts


def butterfly(
    n, table_hbm, mask_hbm, w_hbm, bias_hbm, out_ref,
    table_ref, mask_ref, bias_ref,
    tally, planes, prefix, raw, hold, came, joined, w_ref, wcat,
    send_sem, recv_sem, raw_send, raw_recv, count_send, count_recv, plane_send, plane_recv, load_sem,
):
    half, height = table_hbm.shape
    width = out_ref.shape[1]
    lines = height // 128
    levels = (n - 1).bit_length()
    lanes = height // CHUNKS
    side = min(PLANE, n)
    crowd = min(RAW, n)
    first = (crowd - 1).bit_length()
    count_planes = n // side
    me = lax.axis_index("rows")
    core = lax.axis_index("section")
    plane = me // side
    seat = lax.rem(me, side)

    columns = pl.ds(pl.multiple_of(core * width, 128), width)
    mask_copy = pltpu.make_async_copy(mask_hbm, mask_ref, load_sem.at[0])
    table_copy = pltpu.make_async_copy(table_hbm, table_ref, load_sem.at[1])
    w_copy = pltpu.make_async_copy(w_hbm.at[:, columns], w_ref, load_sem.at[2])
    bias_copy = pltpu.make_async_copy(bias_hbm.at[:, columns], bias_ref, load_sem.at[3])
    for load in (mask_copy, table_copy, w_copy, bias_copy):
        load.start()

    def seat_peer(step):
        return plane * side + lax.rem(seat + step, side)

    def plane_peer(step):
        return lax.rem(plane + step, count_planes) * side + seat

    barrier = pltpu.get_barrier_semaphore()
    for step in range(1, side):
        pl.semaphore_signal(barrier, inc=1, device_id={"rows": seat_peer(step)})
    for step in range(1, count_planes):
        pl.semaphore_signal(barrier, inc=1, device_id={"rows": plane_peer(step)})
    pl.semaphore_signal(barrier, inc=1, device_id={"section": 1 - core})

    mask_copy.wait()
    mask = mask_ref[...]
    ones = mask.astype(F32).astype(BF16)
    row = lax.broadcasted_iota(I32, (128, 128), 0)
    col = lax.broadcasted_iota(I32, (128, 128), 1)
    before = jnp.where(row < col, 1.0, 0.0).astype(BF16)
    inner = jnp.dot(ones, before, preferred_element_type=F32).astype(I32)
    sums = jnp.dot(ones, jnp.ones((128, 128), BF16), preferred_element_type=F32).astype(I32)
    running = jnp.zeros((1, 128), I32)
    starts = []
    for line in range(lines):
        starts.append(running)
        running = running + sums[line : line + 1]
    tally[seat] = running
    slot = jnp.where(mask == 1, inner + jnp.concatenate(starts, 0), -1)

    own = lax.rem(me, crowd)
    table_copy.wait()
    turned = jnp.concatenate(split(table_ref[...], 3), 0)
    for chunk in range(CHUNKS):
        here = chunk * lanes + lax.broadcasted_iota(I32, (lanes, 128), 0)
        hot = jnp.concatenate(
            [jnp.where(here == slot[b : b + 1], 1.0, 0.0).astype(BF16) for b in range(chunk * lanes // 128, lines)], 1
        )
        folded = lax.dot_general(
            turned[:, chunk * lanes :], hot, (((1,), (1,)), ((), ())), preferred_element_type=F32
        )
        raw[own, :, chunk * lanes : (chunk + 1) * lanes] = (
            folded[:half] + folded[half : 2 * half]
        ) + folded[2 * half :]

    pl.semaphore_wait(barrier, side + count_planes - 1)

    def seat_copy(step):
        return pltpu.make_async_remote_copy(
            src_ref=tally.at[seat], dst_ref=tally.at[seat],
            send_sem=count_send.at[step], recv_sem=count_recv.at[step],
            device_id={"rows": seat_peer(step)},
        )

    def plane_copy(step):
        return pltpu.make_async_remote_copy(
            src_ref=planes.at[plane], dst_ref=planes.at[plane],
            send_sem=plane_send.at[step], recv_sem=plane_recv.at[step],
            device_id={"rows": plane_peer(step)},
        )

    def raw_copy(step):
        return pltpu.make_async_remote_copy(
            src_ref=raw.at[own], dst_ref=raw.at[own],
            send_sem=raw_send.at[step], recv_sem=raw_recv.at[step],
            device_id={"rows": me - own + lax.rem(own + step, crowd)},
        )

    for step in range(1, side):
        seat_copy(step).start()
    for step in range(1, crowd):
        raw_copy(step).start()
    for step in range(1, side):
        seat_copy(step).wait_recv()
    everyone = jnp.zeros((1, 128), I32)
    for at in range(side):
        everyone = everyone + tally[at]
    planes[plane] = everyone
    for step in range(1, count_planes):
        plane_copy(step).start()

    w_copy.wait()
    bias_copy.wait()
    bias = bias_ref[...]
    w_hi, w_lo = split(w_ref[...], 2)
    b_hi, b_mid, b_lo = [part.astype(F32) for part in split(bias, 3)]
    line = lax.broadcasted_iota(I32, (16, width), 0)
    extra = jnp.where(line == 0, b_hi, jnp.where(line == 1, b_mid, jnp.where(line == 2, b_lo, 0.0)))
    wcat[...] = jnp.concatenate([w_hi, w_lo, w_hi, extra.astype(BF16)], 0)

    for step in range(1, count_planes):
        plane_copy(step).wait_recv()
    total = jnp.zeros((1, 128), I32)
    for at in range(count_planes):
        prefix[at * side] = total
        total = total + planes[at]
    prefix[n] = total
    running = prefix[plane * side]
    for at in range(side - 1):
        running = running + tally[at]
        prefix[plane * side + at + 1] = running

    def wide(x):
        return jnp.concatenate([x] * (lanes // 128), 1)

    def data_copy(level, chunk):
        at = (slice(None), pl.ds(chunk * lanes, lanes))
        return pltpu.make_async_remote_copy(
            src_ref=hold.at[(level,) + at], dst_ref=came.at[(level,) + at],
            send_sem=send_sem.at[level, chunk], recv_sem=recv_sem.at[level, chunk],
            device_id={"rows": me + (1 - 2 * (me // (1 << level) % 2)) * (1 << level)},
        )

    def join_copy(chunk):
        at = (core, slice(None), pl.ds(chunk * lanes, lanes))
        return pltpu.make_async_remote_copy(
            src_ref=joined.at[at], dst_ref=joined.at[at],
            send_sem=send_sem.at[levels, chunk], recv_sem=recv_sem.at[levels, chunk],
            device_id={"section": 1 - core},
        )

    for step in range(1, crowd):
        raw_copy(step).wait_recv()
    turns = []
    for at in range(crowd):
        shift = (prefix[me - own + at] & (height - 1))[0, 0]
        turns.append(pltpu.roll(raw[at], shift, 1))
    low = wide(prefix[me - own])
    for chunk in range(CHUNKS):
        at = slice(chunk * lanes, (chunk + 1) * lanes)
        base = own * height + chunk * lanes + lax.broadcasted_iota(I32, (1, lanes), 1)
        place = low + ((base - low) & (crowd * height - 1))
        place = jnp.broadcast_to(place, (half, lanes))
        block = turns[0][:, at]
        for other in range(1, crowd):
            block = jnp.where(place >= wide(prefix[me - own + other]), turns[other][:, at], block)
        hold[first, :, at] = block
        data_copy(first, chunk).start()

    for level in range(first, levels):
        reach = 2 << level
        group = me // reach * reach
        bit = me // (1 << level) % 2
        low = wide(prefix[group])
        middle = wide(prefix[group + (1 << level)])
        for chunk in range(CHUNKS):
            at = slice(chunk * lanes, (chunk + 1) * lanes)
            data_copy(level, chunk).wait_recv()
            base = (me % reach) * height + chunk * lanes
            base = base + lax.broadcasted_iota(I32, (1, lanes), 1)
            place = low + ((base - low) & (reach * height - 1))
            upper = jnp.where(place >= middle, 1, 0)
            foreign = jnp.broadcast_to(upper, (half, lanes)) != bit
            block = jnp.where(foreign, came[level, :, at], hold[level, :, at])
            if level < levels - 1:
                hold[level + 1, :, at] = block
                data_copy(level + 1, chunk).start()
            else:
                joined[core, :, at] = block
                join_copy(chunk).start()

    ends = wide(total)
    for chunk in range(CHUNKS):
        at = slice(chunk * lanes, (chunk + 1) * lanes)
        join_copy(chunk).wait_recv()
        owned = me * height + chunk * lanes + lax.broadcasted_iota(I32, (1, lanes), 1)
        filled = jnp.where(owned < ends, 1.0, 0.0)
        rows = jnp.concatenate([joined[0, :, at], joined[1, :, at]], 0)
        rows = jnp.where(jnp.broadcast_to(filled, rows.shape) > 0.5, rows, 0.0)
        a_hi, a_lo = split(rows, 2)
        marks = jnp.broadcast_to(filled, (16, lanes)).astype(BF16)
        lhs = jnp.concatenate([a_hi, a_hi, a_lo, marks], 0)
        out_ref[at, :] = lax.dot_general(
            lhs, wcat[...], (((0,), (0,)), ((), ())), preferred_element_type=F32
        ).astype(BF16)

    for step in range(1, side):
        seat_copy(step).wait_send()
    for step in range(1, count_planes):
        plane_copy(step).wait_send()
    for step in range(1, crowd):
        raw_copy(step).wait_send()
    for level in range(first, levels):
        for chunk in range(CHUNKS):
            data_copy(level, chunk).wait_send()
    for chunk in range(CHUNKS):
        join_copy(chunk).wait_send()


def wide(x, lanes):
    return jnp.concatenate([x] * (lanes // 128), 1)


def flip(at, step, extent):
    out, bit = 0, 1
    while bit < extent:
        a, b = at // bit % 2, step // bit % 2
        out = out + bit * (a + b - 2 * a * b)
        bit *= 2
    return out


def direct(
    n, table_hbm, mask_hbm, w_hbm, bias_hbm, out_ref,
    table_ref, mask_ref, bias_ref,
    tally, prefix, gather, heap, pieces, parts, got, came, joined, w_ref, wcat,
    load_sem, send, count_recv, line_recv, gather_recv, heap_recv, piece_recv, across_recv, join_recv, ready,
):
    half, height = table_hbm.shape
    width = out_ref.shape[1]
    rows = height // 128
    lanes = height // CHUNKS
    groups = half // GROUP
    side = min(PLANE, n)
    lines = n // side
    me = lax.axis_index("rows")
    core = lax.axis_index("section")
    line = me // side
    seat = lax.rem(me, side)
    flat = core == 1

    columns = pl.ds(pl.multiple_of(core * width, 128), width)
    mask_copy = pltpu.make_async_copy(mask_hbm, mask_ref, load_sem.at[0])
    table_copy = pltpu.make_async_copy(table_hbm, table_ref, load_sem.at[1])
    w_copy = pltpu.make_async_copy(w_hbm.at[:, columns], w_ref, load_sem.at[2])
    bias_copy = pltpu.make_async_copy(bias_hbm.at[:, columns], bias_ref, load_sem.at[3])
    for load in (mask_copy, table_copy, w_copy, bias_copy):
        load.start()

    barrier = pltpu.get_barrier_semaphore()
    pl.semaphore_signal(barrier, inc=1, device_id={"section": 1 - core})

    def tells(source, target):
        return source != target and not (source == 0 and target > 1)

    def later(source, target):
        return source < 2 and target > source

    def far(source, target):
        return source > 1 and target == 0

    @pl.when(flat)
    def _():
        for step in range(1, side):
            pl.semaphore_signal(barrier, inc=1, device_id={"rows": line * side + flip(seat, step, side)})
        for other in range(lines):
            for z in range(lines):
                if tells(other, z) and not later(other, z):
                    @pl.when(line == z)
                    def _(other=other):
                        pl.semaphore_signal(barrier, inc=1, device_id={"rows": other * side + seat})
            for z in range(other):
                @pl.when(line == z)
                def _(other=other, z=z):
                    for at in range(side) if far(other, z) else [seat]:
                        pl.semaphore_signal(barrier, inc=1, device_id={"rows": other * side + at, "section": 0})

    mask_copy.wait()
    mask = mask_ref[...]
    ones = mask.astype(F32).astype(BF16)
    row = lax.broadcasted_iota(I32, (128, 128), 0)
    col = lax.broadcasted_iota(I32, (128, 128), 1)
    before = jnp.where(row < col, 1.0, 0.0).astype(BF16)
    inner = jnp.dot(ones, before, preferred_element_type=F32).astype(I32)
    sums = jnp.dot(ones, jnp.ones((128, 128), BF16), preferred_element_type=F32).astype(I32)
    running = jnp.zeros((1, 128), I32)
    starts = []
    for at in range(rows):
        starts.append(running)
        running = running + sums[at : at + 1]
    tally[me] = running
    slot = jnp.where(mask == 1, inner + jnp.concatenate(starts, 0), -1)

    def far_count():
        at = tally.at[me]
        return [
            pltpu.make_async_remote_copy(
                src_ref=at, dst_ref=at, send_sem=send.at[0], recv_sem=count_recv.at[2],
                device_id={"rows": to, "section": 1},
            )
            for to in range(side)
        ]

    for z in range(lines):
        @pl.when(jnp.logical_and(core == 0, line == z))
        def _(z=z):
            pl.semaphore_wait(barrier, 1 + z + (side - 1 if z > 1 else 0))
            if z > 1:
                for copy in far_count():
                    copy.start()

    def seat_count():
        at = tally.at[me]
        return [
            pltpu.make_async_remote_copy(
                src_ref=at, dst_ref=at, send_sem=send.at[0], recv_sem=count_recv.at[0],
                device_id={"rows": line * side + flip(seat, step, side)},
            )
            for step in range(1, side)
        ]

    def enter(z):
        ahead = sum(tells(z, other) and not later(z, other) for other in range(lines))
        pl.semaphore_wait(barrier, side + ahead)
        for other in range(min(z, 2)):
            if tells(other, z):
                pl.semaphore_signal(ready, inc=1, device_id={"rows": other * side + seat})
        for copy in seat_count():
            copy.start()

    for z in range(min(lines, 2)):
        @pl.when(jnp.logical_and(flat, line == z))
        def _(z=z):
            enter(z)

    own = jnp.where(flat, seat, line)
    table_copy.wait()
    terms = jnp.concatenate(split(table_ref[...], TERMS), 0)
    for chunk in range(CHUNKS):
        here = chunk * lanes + lax.broadcasted_iota(I32, (lanes, 128), 0)
        hot = jnp.concatenate(
            [jnp.where(here == slot[b : b + 1], 1.0, 0.0).astype(BF16) for b in range(chunk * lanes // 128, rows)], 1
        )
        folded = lax.dot_general(
            terms[:, chunk * lanes :], hot, (((1,), (1,)), ((), ())), preferred_element_type=F32
        )
        block = folded[:half]
        for term in range(1, TERMS):
            block = block + folded[term * half : (term + 1) * half]
        gather[own, :, chunk * lanes : (chunk + 1) * lanes] = block

    def span(g):
        return pl.ds(g * GROUP, GROUP)

    def remote(src, dst, send, recv, **to):
        return pltpu.make_async_remote_copy(src_ref=src, dst_ref=dst, send_sem=send, recv_sem=recv, device_id=to)

    def line_count(source, target):
        low = 0 if target > source == 1 else source * side
        at = tally.at[pl.ds(low, (source + 1) * side - low)]
        return remote(
            at, at, send.at[0], line_recv.at[1 if target < source else 0], rows=target * side + seat
        )

    def total_copy():
        at = prefix.at[n]
        return remote(at, at, send.at[0], count_recv.at[1], section=1 - core)

    def seat_copy(step, g):
        at = gather.at[seat, span(g)]
        to = line * side + flip(seat, step, side)
        return remote(at, at, send.at[0], gather_recv.at[g], rows=to)

    def line_copy(source, target, g):
        return remote(
            gather.at[source, span(g)], heap.at[source, span(g)],
            send.at[0], heap_recv.at[g], rows=target * side + seat, section=1,
        )

    def order(source):
        every = range(groups)
        first = [(0, g) for g in every] if source else []
        near = [(target, g) for target in reversed(range(2, source)) for g in every]
        after = [(source, g) for g in every] + [(1, g) for g in every if source == 2 and g >= LIFT]
        return first[:EARLY] + near + first[EARLY:] + after

    def lift_copy(g):
        at = heap.at[2, span(g)]
        return remote(at, at, send.at[0], heap_recv.at[g], rows=side + seat)

    def pass_copy(g):
        at = heap.at[3, span(g)]
        return remote(at, at, send.at[0], heap_recv.at[g], rows=side + seat)

    def down_copy(source, target, g):
        return remote(
            pieces.at[target, span(g)], got.at[source, span(g)],
            send.at[0], piece_recv.at[g], rows=target * side + seat,
        )

    def across_copy(step, g):
        return remote(
            parts.at[step, span(g)], came.at[step, span(g)],
            send.at[0], across_recv.at[g], rows=line * side + flip(seat, step, side),
        )

    def join_copy(which, g):
        at = joined.at[which, span(g)]
        return remote(at, at, send.at[0], join_recv.at[0], section=1 - core)

    def arrived(count, g, sem):
        at = heap.at[pl.ds(0, count), span(g)]
        remote(at, at, sem, sem, section=core).wait_recv()

    def left(count, sem):
        at = heap.at[pl.ds(0, count)]
        remote(at, at, sem, sem, section=core).wait_send()

    def told(count, sem):
        at = tally.at[pl.ds(0, count)]
        remote(at, at, sem, sem, section=core).wait_recv()

    def said(count, sem):
        at = tally.at[pl.ds(0, count)]
        remote(at, at, sem, sem, section=core).wait_send()

    def extend(start, stop):
        running = prefix[start] if start else jnp.zeros((1, 128), I32)
        prefix[start] = running
        for at in range(start, stop):
            running = running + tally[at]
            prefix[at + 1] = running

    for z in range(2, lines):
        @pl.when(jnp.logical_and(flat, line == z))
        def _(z=z):
            enter(z)

    @pl.when(flat)
    def _():
        for g in range(groups):
            for step in range(1, side):
                seat_copy(step, g).start()

    for source in range(lines):
        @pl.when(jnp.logical_and(core == 0, line == source))
        def _(source=source):
            for target, g in order(source):
                line_copy(source, target, g).start()

    w_copy.wait()
    bias_copy.wait()
    bias = bias_ref[...]
    w_hi, w_lo = split(w_ref[...], 2)
    b_hi, b_mid, b_lo = [part.astype(F32) for part in split(bias, 3)]
    at = lax.broadcasted_iota(I32, (16, width), 0)
    extra = jnp.where(at == 0, b_hi, jnp.where(at == 1, b_mid, jnp.where(at == 2, b_lo, 0.0)))
    wcat[...] = jnp.concatenate([w_hi, w_lo, w_hi, extra.astype(BF16)], 0)

    lane = lax.broadcasted_iota(I32, (GROUP, height), 1)

    def bound(index):
        return wide(jnp.broadcast_to(prefix[index], (GROUP, 128)), height)

    def turn(ref, slot, index, g):
        shift = (prefix[index] & (height - 1))[0, 0]
        return pltpu.roll(ref[slot, g * GROUP : (g + 1) * GROUP], shift, 1)

    def routed(z):
        base = seat * height + lane
        told(side - 1, count_recv.at[0])
        for target in range(z):
            if not far(z, target):
                line_count(z, target).start()
        if z == 1:
            told(side, line_recv.at[0])
        above = [target for target in range(z + 1, lines) if tells(z, target)]
        if z < 2 and above:
            pl.semaphore_wait(ready, len(above))
        for target in above:
            line_count(z, target).start()
        if z > 1:
            told(z * side, line_recv.at[0])
        extend(0, (z + 1) * side)
        low, high = bound(z * side), bound(z * side + side)
        relayed = z == 3
        merges = z == 2 and lines > 3
        if merges:
            for g in range(groups):
                arrived(lines - z, g, heap_recv.at[g])
                pass_copy(g).start()
        for g in range(groups):
            at_g = slice(g * GROUP, (g + 1) * GROUP)
            arrived(side - 1, g, gather_recv.at[g])
            blocks = [turn(gather, at, z * side + at, g) for at in range(side)]

            def choose(place):
                piece = jnp.where(place >= low, blocks[0], 0.0)
                for at in range(1, side):
                    piece = jnp.where(place >= bound(z * side + at), blocks[at], piece)
                return jnp.where(place >= high, 0.0, piece)

            if relayed:
                mixed = choose(low + ((base - low) & (side * height - 1)))
                pieces[2, at_g] = mixed
                down_copy(3, 2, g).start()
                joined[1, at_g] = jnp.where(z * side * height + base < low + side * height, mixed, 0.0)
            else:
                for target in range(z):
                    pieces[target, at_g] = choose(target * side * height + base)
                    if not merges:
                        down_copy(z, target, g).start()
                joined[1, at_g] = choose(z * side * height + base)
            if relayed:
                join_copy(1, g).start()
        above = sum(not far(source, z) for source in range(z + 1, lines))
        if above:
            told(above * side, line_recv.at[1])
        if z == 0 and lines > 2:
            told((lines - 2) * side, count_recv.at[2])
        extend((z + 1) * side, n)
        total_copy().start()
        def merge():
            for g in range(groups):
                at_g = slice(g * GROUP, (g + 1) * GROUP)
                arrived(1, g, piece_recv.at[g])
                for target in range(3):
                    place = target * side * height + base
                    inside = jnp.logical_and(place >= high, place < high + side * height)
                    block = jnp.where(inside, got[3, at_g], joined[1, at_g] if target == 2 else pieces[target, at_g])
                    if target == 2:
                        joined[1, at_g] = block
                        join_copy(1, g).start()
                    else:
                        pieces[target, at_g] = block
                        if target == 0:
                            down_copy(2, 0, g).start()
            for g in range(groups):
                down_copy(2, 1, g).start()

        sources = range(z, lines)
        for g in range(groups):
            if merges and g == MERGE:
                merge()
            at_g = slice(g * GROUP, (g + 1) * GROUP)
            if not merges:
                arrived(lines - z, g, heap_recv.at[g])
            if z == 0 and lines > 2 and g < LIFT:
                lift_copy(g).start()
            turned = [turn(heap, at, at * side + seat, g) for at in sources]
            for step in [*range(1, side), 0]:
                place = (z * side + flip(seat, step, side)) * height + lane
                piece = jnp.zeros((GROUP, height), F32)
                for at, block in zip(sources, turned):
                    index = at * side + seat
                    inside = jnp.logical_and(place >= bound(index), place < bound(index + 1))
                    piece = jnp.where(inside, block, piece)
                if step:
                    parts[step, at_g] = piece
                    across_copy(step, g).start()
                else:
                    joined[0, at_g] = piece
        def take_flat(g):
            froms = range(z + 1, min(lines, 3))
            at_g = slice(g * GROUP, (g + 1) * GROUP)
            if froms:
                arrived(len(froms), g, piece_recv.at[g])
                block = joined[1, at_g]
                for source in froms:
                    block = block + got[source, at_g]
                joined[1, at_g] = block
            join_copy(1, g).start()

        def take_tall(g):
            at_g = slice(g * GROUP, (g + 1) * GROUP)
            arrived(side - 1, g, across_recv.at[g])
            block = joined[0, at_g]
            for step in range(1, side):
                block = block + came[step, at_g]
            joined[0, at_g] = block
            join_copy(0, g).start()

        for g in range(groups):
            take_tall(g)
            if not merges and not relayed:
                take_flat(g)

    for z in range(lines):
        @pl.when(jnp.logical_and(flat, line == z))
        def _(z=z):
            routed(z)

    @pl.when(core == 0)
    def _():
        at = prefix.at[n]
        remote(at, at, send.at[0], count_recv.at[1], section=1 - core).wait_recv()
        remote(joined, joined, send.at[0], join_recv.at[0], section=1 - core).wait_recv()

    ends = wide(prefix[n], lanes)
    for chunk in range(CHUNKS):
        at = slice(chunk * lanes, (chunk + 1) * lanes)
        owned = me * height + chunk * lanes + lax.broadcasted_iota(I32, (1, lanes), 1)
        filled = jnp.where(owned < ends, 1.0, 0.0)
        block = jnp.concatenate([joined[0, :, at], joined[1, :, at]], 0)
        a_hi, a_lo = split(block, 2)
        marks = jnp.broadcast_to(filled, (16, lanes)).astype(BF16)
        lhs = jnp.concatenate([a_hi, a_hi, a_lo, marks], 0)
        out_ref[at, :] = lax.dot_general(
            lhs, wcat[...], (((0,), (0,)), ((), ())), preferred_element_type=F32
        ).astype(BF16)

    for z in range(lines):
        @pl.when(jnp.logical_and(flat, line == z))
        def _(z=z):
            said(side - 1, send.at[0])
            below = sum(not far(z, target) for target in range(z))
            if below:
                said(below * side, send.at[0])
            above = sum(tells(z, target) for target in range(z + 1, lines))
            if above:
                said(above * side * (2 if z == 1 else 1), send.at[0])
            total_copy().wait_send()
            left(side - 1, send.at[0])
            if z == 2 and lines > 3:
                left(1, send.at[0])
            if z:
                left(1 if z == 3 else z, send.at[0])
            elif lines > 2:
                for g in range(LIFT):
                    lift_copy(g).wait_send()
            left(side - 1, send.at[0])
            left(2, send.at[0])

        @pl.when(jnp.logical_and(core == 0, line == z))
        def _(z=z):
            for target, g in order(z):
                line_copy(z, target, g).wait_send()
            if z > 1:
                said(side, send.at[0])


def solution(mesh):
    n, sections = mesh.shape["rows"], mesh.shape["section"]

    def step(table, mask, weight, bias):
        height, half = table.shape
        cols, features = weight.shape
        width = features // sections
        levels = (n - 1).bit_length()
        side, crowd = min(PLANE, n), min(RAW, n)
        lines, groups = n // side, half // GROUP
        operands = table.T, mask.reshape(height // 128, 128), weight, bias.reshape(1, features)
        sem = pltpu.SemaphoreType.DMA
        loads = [
            pltpu.VMEM((half, height), F32),
            pltpu.VMEM((height // 128, 128), I32),
            pltpu.VMEM((1, width), F32),
        ]
        weights = [
            pltpu.VMEM((cols, width), F32),
            pltpu.VMEM((3 * cols + 16, width), BF16),
        ]
        if lines <= LINES:
            most = max(side, lines)
            block = pltpu.VMEM((most, half, height), F32)
            body = direct
            scratch = loads + [
                pltpu.VMEM((n, 1, 128), I32),
                pltpu.VMEM((n + 1, 1, 128), I32),
                block, block, block, block, block, block,
                pltpu.VMEM((sections, half, height), F32),
            ] + weights + [
                sem((4,)), sem((1,)), sem((3,)), sem((2,)),
                sem((groups,)), sem((groups,)), sem((groups,)), sem((groups,)),
                sem((1,)), pltpu.SemaphoreType.REGULAR,
            ]
        else:
            body = butterfly
            scratch = loads + [
                pltpu.VMEM((side, 1, 128), I32),
                pltpu.VMEM((n // side, 1, 128), I32),
                pltpu.VMEM((n + 1, 1, 128), I32),
                pltpu.VMEM((crowd, half, height), F32),
                pltpu.VMEM((levels, half, height), F32),
                pltpu.VMEM((levels, half, height), F32),
                pltpu.VMEM((sections, half, height), F32),
            ] + weights + [
                sem((levels + 1, CHUNKS)), sem((levels + 1, CHUNKS)),
                sem((crowd,)), sem((crowd,)),
                sem((side,)), sem((side,)),
                sem((n // side,)), sem((n // side,)),
                sem((4,)),
            ]
        return pl.pallas_call(
            functools.partial(body, n),
            name="filter_project",
            out_shape=jax.ShapeDtypeStruct((height, width), BF16),
            in_specs=[pl.BlockSpec(memory_space=pltpu.HBM)] * 4,
            out_specs=pl.BlockSpec(memory_space=pltpu.VMEM),
            scratch_shapes=scratch,
            compiler_params=pltpu.CompilerParams(
                collective_id=0, has_side_effects=True, vmem_limit_bytes=16 << 20
            ),
        )(*[pltpu.with_memory_space_constraint(x, pltpu.HBM) for x in operands])

    return jax.shard_map(
        step,
        mesh=mesh,
        in_specs=(P("rows", "section"), P("rows"), P(), P()),
        out_specs=P("rows", "section"),
        check_vma=False,
    )
```

```python
import functools

import jax
import jax.numpy as jnp
from jax import lax
from jax.experimental import pallas as pl
from jax.experimental.pallas import tpu as pltpu
from jax.sharding import PartitionSpec as P

CHUNKS = 4
PLANE = 4
RAW = 4
LINES = 4
GROUP = 8
TERMS = 2
MERGE = 1
EARLY = 3
LIFT = 1
F32 = jnp.float32
BF16 = jnp.bfloat16
I32 = jnp.int32


def split(x, terms):
    parts = []
    for _ in range(terms):
        part = x.astype(BF16)
        parts.append(part)
        x = x - part.astype(F32)
    return parts


def butterfly(
    n, table_hbm, mask_hbm, w_hbm, bias_hbm, out_ref,
    table_ref, mask_ref, bias_ref,
    tally, planes, prefix, raw, hold, came, joined, w_ref, wcat,
    send_sem, recv_sem, raw_send, raw_recv, count_send, count_recv, plane_send, plane_recv, load_sem,
):
    half, height = table_hbm.shape
    width = out_ref.shape[1]
    lines = height // 128
    levels = (n - 1).bit_length()
    lanes = height // CHUNKS
    side = min(PLANE, n)
    crowd = min(RAW, n)
    first = (crowd - 1).bit_length()
    count_planes = n // side
    me = lax.axis_index("rows")
    core = lax.axis_index("section")
    plane = me // side
    seat = lax.rem(me, side)

    columns = pl.ds(pl.multiple_of(core * width, 128), width)
    mask_copy = pltpu.make_async_copy(mask_hbm, mask_ref, load_sem.at[0])
    table_copy = pltpu.make_async_copy(table_hbm, table_ref, load_sem.at[1])
    w_copy = pltpu.make_async_copy(w_hbm.at[:, columns], w_ref, load_sem.at[2])
    bias_copy = pltpu.make_async_copy(bias_hbm.at[:, columns], bias_ref, load_sem.at[3])
    for load in (mask_copy, table_copy, w_copy, bias_copy):
        load.start()

    def seat_peer(step):
        return plane * side + lax.rem(seat + step, side)

    def plane_peer(step):
        return lax.rem(plane + step, count_planes) * side + seat

    barrier = pltpu.get_barrier_semaphore()
    for step in range(1, side):
        pl.semaphore_signal(barrier, inc=1, device_id={"rows": seat_peer(step)})
    for step in range(1, count_planes):
        pl.semaphore_signal(barrier, inc=1, device_id={"rows": plane_peer(step)})
    pl.semaphore_signal(barrier, inc=1, device_id={"section": 1 - core})

    mask_copy.wait()
    mask = mask_ref[...]
    ones = mask.astype(F32).astype(BF16)
    row = lax.broadcasted_iota(I32, (128, 128), 0)
    col = lax.broadcasted_iota(I32, (128, 128), 1)
    before = jnp.where(row < col, 1.0, 0.0).astype(BF16)
    inner = jnp.dot(ones, before, preferred_element_type=F32).astype(I32)
    sums = jnp.dot(ones, jnp.ones((128, 128), BF16), preferred_element_type=F32).astype(I32)
    running = jnp.zeros((1, 128), I32)
    starts = []
    for line in range(lines):
        starts.append(running)
        running = running + sums[line : line + 1]
    tally[seat] = running
    slot = jnp.where(mask == 1, inner + jnp.concatenate(starts, 0), -1)

    own = lax.rem(me, crowd)
    table_copy.wait()
    turned = jnp.concatenate(split(table_ref[...], 3), 0)
    for chunk in range(CHUNKS):
        here = chunk * lanes + lax.broadcasted_iota(I32, (lanes, 128), 0)
        hot = jnp.concatenate(
            [jnp.where(here == slot[b : b + 1], 1.0, 0.0).astype(BF16) for b in range(chunk * lanes // 128, lines)], 1
        )
        folded = lax.dot_general(
            turned[:, chunk * lanes :], hot, (((1,), (1,)), ((), ())), preferred_element_type=F32
        )
        raw[own, :, chunk * lanes : (chunk + 1) * lanes] = (
            folded[:half] + folded[half : 2 * half]
        ) + folded[2 * half :]

    pl.semaphore_wait(barrier, side + count_planes - 1)

    def seat_copy(step):
        return pltpu.make_async_remote_copy(
            src_ref=tally.at[seat], dst_ref=tally.at[seat],
            send_sem=count_send.at[step], recv_sem=count_recv.at[step],
            device_id={"rows": seat_peer(step)},
        )

    def plane_copy(step):
        return pltpu.make_async_remote_copy(
            src_ref=planes.at[plane], dst_ref=planes.at[plane],
            send_sem=plane_send.at[step], recv_sem=plane_recv.at[step],
            device_id={"rows": plane_peer(step)},
        )

    def raw_copy(step):
        return pltpu.make_async_remote_copy(
            src_ref=raw.at[own], dst_ref=raw.at[own],
            send_sem=raw_send.at[step], recv_sem=raw_recv.at[step],
            device_id={"rows": me - own + lax.rem(own + step, crowd)},
        )

    for step in range(1, side):
        seat_copy(step).start()
    for step in range(1, crowd):
        raw_copy(step).start()
    for step in range(1, side):
        seat_copy(step).wait_recv()
    everyone = jnp.zeros((1, 128), I32)
    for at in range(side):
        everyone = everyone + tally[at]
    planes[plane] = everyone
    for step in range(1, count_planes):
        plane_copy(step).start()

    w_copy.wait()
    bias_copy.wait()
    bias = bias_ref[...]
    w_hi, w_lo = split(w_ref[...], 2)
    b_hi, b_mid, b_lo = [part.astype(F32) for part in split(bias, 3)]
    line = lax.broadcasted_iota(I32, (16, width), 0)
    extra = jnp.where(line == 0, b_hi, jnp.where(line == 1, b_mid, jnp.where(line == 2, b_lo, 0.0)))
    wcat[...] = jnp.concatenate([w_hi, w_lo, w_hi, extra.astype(BF16)], 0)

    for step in range(1, count_planes):
        plane_copy(step).wait_recv()
    total = jnp.zeros((1, 128), I32)
    for at in range(count_planes):
        prefix[at * side] = total
        total = total + planes[at]
    prefix[n] = total
    running = prefix[plane * side]
    for at in range(side - 1):
        running = running + tally[at]
        prefix[plane * side + at + 1] = running

    def wide(x):
        return jnp.concatenate([x] * (lanes // 128), 1)

    def data_copy(level, chunk):
        at = (slice(None), pl.ds(chunk * lanes, lanes))
        return pltpu.make_async_remote_copy(
            src_ref=hold.at[(level,) + at], dst_ref=came.at[(level,) + at],
            send_sem=send_sem.at[level, chunk], recv_sem=recv_sem.at[level, chunk],
            device_id={"rows": me + (1 - 2 * (me // (1 << level) % 2)) * (1 << level)},
        )

    def join_copy(chunk):
        at = (core, slice(None), pl.ds(chunk * lanes, lanes))
        return pltpu.make_async_remote_copy(
            src_ref=joined.at[at], dst_ref=joined.at[at],
            send_sem=send_sem.at[levels, chunk], recv_sem=recv_sem.at[levels, chunk],
            device_id={"section": 1 - core},
        )

    for step in range(1, crowd):
        raw_copy(step).wait_recv()
    turns = []
    for at in range(crowd):
        shift = (prefix[me - own + at] & (height - 1))[0, 0]
        turns.append(pltpu.roll(raw[at], shift, 1))
    low = wide(prefix[me - own])
    for chunk in range(CHUNKS):
        at = slice(chunk * lanes, (chunk + 1) * lanes)
        base = own * height + chunk * lanes + lax.broadcasted_iota(I32, (1, lanes), 1)
        place = low + ((base - low) & (crowd * height - 1))
        place = jnp.broadcast_to(place, (half, lanes))
        block = turns[0][:, at]
        for other in range(1, crowd):
            block = jnp.where(place >= wide(prefix[me - own + other]), turns[other][:, at], block)
        hold[first, :, at] = block
        data_copy(first, chunk).start()

    for level in range(first, levels):
        reach = 2 << level
        group = me // reach * reach
        bit = me // (1 << level) % 2
        low = wide(prefix[group])
        middle = wide(prefix[group + (1 << level)])
        for chunk in range(CHUNKS):
            at = slice(chunk * lanes, (chunk + 1) * lanes)
            data_copy(level, chunk).wait_recv()
            base = (me % reach) * height + chunk * lanes
            base = base + lax.broadcasted_iota(I32, (1, lanes), 1)
            place = low + ((base - low) & (reach * height - 1))
            upper = jnp.where(place >= middle, 1, 0)
            foreign = jnp.broadcast_to(upper, (half, lanes)) != bit
            block = jnp.where(foreign, came[level, :, at], hold[level, :, at])
            if level < levels - 1:
                hold[level + 1, :, at] = block
                data_copy(level + 1, chunk).start()
            else:
                joined[core, :, at] = block
                join_copy(chunk).start()

    ends = wide(total)
    for chunk in range(CHUNKS):
        at = slice(chunk * lanes, (chunk + 1) * lanes)
        join_copy(chunk).wait_recv()
        owned = me * height + chunk * lanes + lax.broadcasted_iota(I32, (1, lanes), 1)
        filled = jnp.where(owned < ends, 1.0, 0.0)
        rows = jnp.concatenate([joined[0, :, at], joined[1, :, at]], 0)
        rows = jnp.where(jnp.broadcast_to(filled, rows.shape) > 0.5, rows, 0.0)
        a_hi, a_lo = split(rows, 2)
        marks = jnp.broadcast_to(filled, (16, lanes)).astype(BF16)
        lhs = jnp.concatenate([a_hi, a_hi, a_lo, marks], 0)
        out_ref[at, :] = lax.dot_general(
            lhs, wcat[...], (((0,), (0,)), ((), ())), preferred_element_type=F32
        ).astype(BF16)

    for step in range(1, side):
        seat_copy(step).wait_send()
    for step in range(1, count_planes):
        plane_copy(step).wait_send()
    for step in range(1, crowd):
        raw_copy(step).wait_send()
    for level in range(first, levels):
        for chunk in range(CHUNKS):
            data_copy(level, chunk).wait_send()
    for chunk in range(CHUNKS):
        join_copy(chunk).wait_send()


def wide(x, lanes):
    return jnp.concatenate([x] * (lanes // 128), 1)


def flip(at, step, extent):
    out, bit = 0, 1
    while bit < extent:
        a, b = at // bit % 2, step // bit % 2
        out = out + bit * (a + b - 2 * a * b)
        bit *= 2
    return out


def direct(
    n, table_hbm, mask_hbm, w_hbm, bias_hbm, out_ref,
    table_ref, mask_ref, bias_ref,
    tally, prefix, gather, heap, pieces, parts, got, came, joined, w_ref, wcat,
    load_sem, send, count_recv, line_recv, gather_recv, heap_recv, piece_recv, across_recv, join_recv, ready,
):
    half, height = table_hbm.shape
    width = out_ref.shape[1]
    rows = height // 128
    lanes = height // CHUNKS
    groups = half // GROUP
    side = min(PLANE, n)
    lines = n // side
    me = lax.axis_index("rows")
    core = lax.axis_index("section")
    line = me // side
    seat = lax.rem(me, side)
    flat = core == 1

    columns = pl.ds(pl.multiple_of(core * width, 128), width)
    mask_copy = pltpu.make_async_copy(mask_hbm, mask_ref, load_sem.at[0])
    table_copy = pltpu.make_async_copy(table_hbm, table_ref, load_sem.at[1])
    w_copy = pltpu.make_async_copy(w_hbm.at[:, columns], w_ref, load_sem.at[2])
    bias_copy = pltpu.make_async_copy(bias_hbm.at[:, columns], bias_ref, load_sem.at[3])
    for load in (mask_copy, table_copy, w_copy, bias_copy):
        load.start()

    barrier = pltpu.get_barrier_semaphore()
    pl.semaphore_signal(barrier, inc=1, device_id={"section": 1 - core})

    def tells(source, target):
        return source != target and not (source == 0 and target > 1)

    def later(source, target):
        return source < 2 and target > source

    def far(source, target):
        return source > 1 and target == 0

    @pl.when(flat)
    def _():
        for step in range(1, side):
            pl.semaphore_signal(barrier, inc=1, device_id={"rows": line * side + flip(seat, step, side)})
        for other in range(lines):
            for z in range(lines):
                if tells(other, z) and not later(other, z):
                    @pl.when(line == z)
                    def _(other=other):
                        pl.semaphore_signal(barrier, inc=1, device_id={"rows": other * side + seat})
            for z in range(other):
                @pl.when(line == z)
                def _(other=other, z=z):
                    for at in range(side) if far(other, z) else [seat]:
                        pl.semaphore_signal(barrier, inc=1, device_id={"rows": other * side + at, "section": 0})

    mask_copy.wait()
    mask = mask_ref[...]
    ones = mask.astype(F32).astype(BF16)
    row = lax.broadcasted_iota(I32, (128, 128), 0)
    col = lax.broadcasted_iota(I32, (128, 128), 1)
    before = jnp.where(row < col, 1.0, 0.0).astype(BF16)
    inner = jnp.dot(ones, before, preferred_element_type=F32).astype(I32)
    sums = jnp.dot(ones, jnp.ones((128, 128), BF16), preferred_element_type=F32).astype(I32)
    running = jnp.zeros((1, 128), I32)
    starts = []
    for at in range(rows):
        starts.append(running)
        running = running + sums[at : at + 1]
    tally[me] = running
    slot = jnp.where(mask == 1, inner + jnp.concatenate(starts, 0), -1)

    def far_count():
        at = tally.at[me]
        return [
            pltpu.make_async_remote_copy(
                src_ref=at, dst_ref=at, send_sem=send.at[0], recv_sem=count_recv.at[2],
                device_id={"rows": to, "section": 1},
            )
            for to in range(side)
        ]

    for z in range(lines):
        @pl.when(jnp.logical_and(core == 0, line == z))
        def _(z=z):
            pl.semaphore_wait(barrier, 1 + z + (side - 1 if z > 1 else 0))
            if z > 1:
                for copy in far_count():
                    copy.start()

    def seat_count():
        at = tally.at[me]
        return [
            pltpu.make_async_remote_copy(
                src_ref=at, dst_ref=at, send_sem=send.at[0], recv_sem=count_recv.at[0],
                device_id={"rows": line * side + flip(seat, step, side)},
            )
            for step in range(1, side)
        ]

    def enter(z):
        ahead = sum(tells(z, other) and not later(z, other) for other in range(lines))
        pl.semaphore_wait(barrier, side + ahead)
        for other in range(min(z, 2)):
            if tells(other, z):
                pl.semaphore_signal(ready, inc=1, device_id={"rows": other * side + seat})
        for copy in seat_count():
            copy.start()

    for z in range(min(lines, 2)):
        @pl.when(jnp.logical_and(flat, line == z))
        def _(z=z):
            enter(z)

    own = jnp.where(flat, seat, line)
    table_copy.wait()
    terms = jnp.concatenate(split(table_ref[...], TERMS), 0)
    for chunk in range(CHUNKS):
        here = chunk * lanes + lax.broadcasted_iota(I32, (lanes, 128), 0)
        hot = jnp.concatenate(
            [jnp.where(here == slot[b : b + 1], 1.0, 0.0).astype(BF16) for b in range(chunk * lanes // 128, rows)], 1
        )
        folded = lax.dot_general(
            terms[:, chunk * lanes :], hot, (((1,), (1,)), ((), ())), preferred_element_type=F32
        )
        block = folded[:half]
        for term in range(1, TERMS):
            block = block + folded[term * half : (term + 1) * half]
        gather[own, :, chunk * lanes : (chunk + 1) * lanes] = block

    def span(g):
        return pl.ds(g * GROUP, GROUP)

    def remote(src, dst, send, recv, **to):
        return pltpu.make_async_remote_copy(src_ref=src, dst_ref=dst, send_sem=send, recv_sem=recv, device_id=to)

    def line_count(source, target):
        low = 0 if target > source == 1 else source * side
        at = tally.at[pl.ds(low, (source + 1) * side - low)]
        return remote(
            at, at, send.at[0], line_recv.at[1 if target < source else 0], rows=target * side + seat
        )

    def total_copy():
        at = prefix.at[n]
        return remote(at, at, send.at[0], count_recv.at[1], section=1 - core)

    def seat_copy(step, g):
        at = gather.at[seat, span(g)]
        to = line * side + flip(seat, step, side)
        return remote(at, at, send.at[0], gather_recv.at[g], rows=to)

    def line_copy(source, target, g):
        return remote(
            gather.at[source, span(g)], heap.at[source, span(g)],
            send.at[0], heap_recv.at[g], rows=target * side + seat, section=1,
        )

    def order(source):
        every = range(groups)
        first = [(0, g) for g in every] if source else []
        near = [(target, g) for target in reversed(range(2, source)) for g in every]
        after = [(source, g) for g in every] + [(1, g) for g in every if source == 2 and g >= LIFT]
        return first[:EARLY] + near + first[EARLY:] + after

    def lift_copy(g):
        at = heap.at[2, span(g)]
        return remote(at, at, send.at[0], heap_recv.at[g], rows=side + seat)

    def pass_copy(g):
        at = heap.at[3, span(g)]
        return remote(at, at, send.at[0], heap_recv.at[g], rows=side + seat)

    def down_copy(source, target, g):
        return remote(
            pieces.at[target, span(g)], got.at[source, span(g)],
            send.at[0], piece_recv.at[g], rows=target * side + seat,
        )

    def across_copy(step, g):
        return remote(
            parts.at[step, span(g)], came.at[step, span(g)],
            send.at[0], across_recv.at[g], rows=line * side + flip(seat, step, side),
        )

    def join_copy(which, g):
        at = joined.at[which, span(g)]
        return remote(at, at, send.at[0], join_recv.at[0], section=1 - core)

    def arrived(count, g, sem):
        at = heap.at[pl.ds(0, count), span(g)]
        remote(at, at, sem, sem, section=core).wait_recv()

    def left(count, sem):
        at = heap.at[pl.ds(0, count)]
        remote(at, at, sem, sem, section=core).wait_send()

    def told(count, sem):
        at = tally.at[pl.ds(0, count)]
        remote(at, at, sem, sem, section=core).wait_recv()

    def said(count, sem):
        at = tally.at[pl.ds(0, count)]
        remote(at, at, sem, sem, section=core).wait_send()

    def extend(start, stop):
        running = prefix[start] if start else jnp.zeros((1, 128), I32)
        prefix[start] = running
        for at in range(start, stop):
            running = running + tally[at]
            prefix[at + 1] = running

    for z in range(2, lines):
        @pl.when(jnp.logical_and(flat, line == z))
        def _(z=z):
            enter(z)

    @pl.when(flat)
    def _():
        for g in range(groups):
            for step in range(1, side):
                seat_copy(step, g).start()

    for source in range(lines):
        @pl.when(jnp.logical_and(core == 0, line == source))
        def _(source=source):
            for target, g in order(source):
                line_copy(source, target, g).start()

    w_copy.wait()
    bias_copy.wait()
    bias = bias_ref[...]
    w_hi, w_lo = split(w_ref[...], 2)
    b_hi, b_mid, b_lo = [part.astype(F32) for part in split(bias, 3)]
    at = lax.broadcasted_iota(I32, (16, width), 0)
    extra = jnp.where(at == 0, b_hi, jnp.where(at == 1, b_mid, jnp.where(at == 2, b_lo, 0.0)))
    wcat[...] = jnp.concatenate([w_hi, w_lo, w_hi, extra.astype(BF16)], 0)

    lane = lax.broadcasted_iota(I32, (GROUP, height), 1)

    def bound(index):
        return wide(jnp.broadcast_to(prefix[index], (GROUP, 128)), height)

    def turn(ref, slot, index, g):
        shift = (prefix[index] & (height - 1))[0, 0]
        return pltpu.roll(ref[slot, g * GROUP : (g + 1) * GROUP], shift, 1)

    def routed(z):
        base = seat * height + lane
        told(side - 1, count_recv.at[0])
        for target in range(z):
            if not far(z, target):
                line_count(z, target).start()
        if z == 1:
            told(side, line_recv.at[0])
        above = [target for target in range(z + 1, lines) if tells(z, target)]
        if z < 2 and above:
            pl.semaphore_wait(ready, len(above))
        for target in above:
            line_count(z, target).start()
        if z > 1:
            told(z * side, line_recv.at[0])
        extend(0, (z + 1) * side)
        low, high = bound(z * side), bound(z * side + side)
        relayed = z == 3
        merges = z == 2 and lines > 3
        for g in range(groups):
            at_g = slice(g * GROUP, (g + 1) * GROUP)
            if merges:
                arrived(lines - z, g, heap_recv.at[g])
                pass_copy(g).start()
            arrived(side - 1, g, gather_recv.at[g])
            blocks = [turn(gather, at, z * side + at, g) for at in range(side)]

            def choose(place):
                piece = jnp.where(place >= low, blocks[0], 0.0)
                for at in range(1, side):
                    piece = jnp.where(place >= bound(z * side + at), blocks[at], piece)
                return jnp.where(place >= high, 0.0, piece)

            if relayed:
                mixed = choose(low + ((base - low) & (side * height - 1)))
                pieces[2, at_g] = mixed
                down_copy(3, 2, g).start()
                joined[1, at_g] = jnp.where(z * side * height + base < low + side * height, mixed, 0.0)
            else:
                for target in range(z):
                    pieces[target, at_g] = choose(target * side * height + base)
                    if not merges:
                        down_copy(z, target, g).start()
                joined[1, at_g] = choose(z * side * height + base)
            if relayed:
                join_copy(1, g).start()
        above = sum(not far(source, z) for source in range(z + 1, lines))
        if above:
            told(above * side, line_recv.at[1])
        if z == 0 and lines > 2:
            told((lines - 2) * side, count_recv.at[2])
        extend((z + 1) * side, n)
        total_copy().start()
        def merge():
            for g in range(groups):
                at_g = slice(g * GROUP, (g + 1) * GROUP)
                arrived(1, g, piece_recv.at[g])
                for target in range(3):
                    place = target * side * height + base
                    inside = jnp.logical_and(place >= high, place < high + side * height)
                    block = jnp.where(inside, got[3, at_g], joined[1, at_g] if target == 2 else pieces[target, at_g])
                    if target == 2:
                        joined[1, at_g] = block
                        join_copy(1, g).start()
                    else:
                        pieces[target, at_g] = block
                        if target == 0:
                            down_copy(2, 0, g).start()
            for g in range(groups):
                down_copy(2, 1, g).start()

        sources = range(z, lines)
        for g in range(groups):
            if merges and g == MERGE:
                merge()
            at_g = slice(g * GROUP, (g + 1) * GROUP)
            if not merges:
                arrived(lines - z, g, heap_recv.at[g])
            if z == 0 and lines > 2 and g < LIFT:
                lift_copy(g).start()
            turned = [turn(heap, at, at * side + seat, g) for at in sources]
            for step in [*range(1, side), 0]:
                place = (z * side + flip(seat, step, side)) * height + lane
                piece = jnp.zeros((GROUP, height), F32)
                for at, block in zip(sources, turned):
                    index = at * side + seat
                    inside = jnp.logical_and(place >= bound(index), place < bound(index + 1))
                    piece = jnp.where(inside, block, piece)
                if step:
                    parts[step, at_g] = piece
                    across_copy(step, g).start()
                else:
                    joined[0, at_g] = piece
        def take_flat(g):
            froms = range(z + 1, min(lines, 3))
            at_g = slice(g * GROUP, (g + 1) * GROUP)
            if froms:
                arrived(len(froms), g, piece_recv.at[g])
                block = joined[1, at_g]
                for source in froms:
                    block = block + got[source, at_g]
                joined[1, at_g] = block
            join_copy(1, g).start()

        def take_tall(g):
            at_g = slice(g * GROUP, (g + 1) * GROUP)
            arrived(side - 1, g, across_recv.at[g])
            block = joined[0, at_g]
            for step in range(1, side):
                block = block + came[step, at_g]
            joined[0, at_g] = block
            join_copy(0, g).start()

        for g in range(groups):
            take_tall(g)
            if not merges and not relayed:
                take_flat(g)

    for z in range(lines):
        @pl.when(jnp.logical_and(flat, line == z))
        def _(z=z):
            routed(z)

    @pl.when(core == 0)
    def _():
        at = prefix.at[n]
        remote(at, at, send.at[0], count_recv.at[1], section=1 - core).wait_recv()
        remote(joined, joined, send.at[0], join_recv.at[0], section=1 - core).wait_recv()

    ends = wide(prefix[n], lanes)
    for chunk in range(CHUNKS):
        at = slice(chunk * lanes, (chunk + 1) * lanes)
        owned = me * height + chunk * lanes + lax.broadcasted_iota(I32, (1, lanes), 1)
        filled = jnp.where(owned < ends, 1.0, 0.0)
        block = jnp.concatenate([joined[0, :, at], joined[1, :, at]], 0)
        a_hi, a_lo = split(block, 2)
        marks = jnp.broadcast_to(filled, (16, lanes)).astype(BF16)
        lhs = jnp.concatenate([a_hi, a_hi, a_lo, marks], 0)
        out_ref[at, :] = lax.dot_general(
            lhs, wcat[...], (((0,), (0,)), ((), ())), preferred_element_type=F32
        ).astype(BF16)

    for z in range(lines):
        @pl.when(jnp.logical_and(flat, line == z))
        def _(z=z):
            said(side - 1, send.at[0])
            below = sum(not far(z, target) for target in range(z))
            if below:
                said(below * side, send.at[0])
            above = sum(tells(z, target) for target in range(z + 1, lines))
            if above:
                said(above * side * (2 if z == 1 else 1), send.at[0])
            total_copy().wait_send()
            left(side - 1, send.at[0])
            if z == 2 and lines > 3:
                left(1, send.at[0])
            if z:
                left(1 if z == 3 else z, send.at[0])
            elif lines > 2:
                for g in range(LIFT):
                    lift_copy(g).wait_send()
            left(side - 1, send.at[0])
            left(2, send.at[0])

        @pl.when(jnp.logical_and(core == 0, line == z))
        def _(z=z):
            for target, g in order(z):
                line_copy(z, target, g).wait_send()
            if z > 1:
                said(side, send.at[0])


def solution(mesh):
    n, sections = mesh.shape["rows"], mesh.shape["section"]

    def step(table, mask, weight, bias):
        height, half = table.shape
        cols, features = weight.shape
        width = features // sections
        levels = (n - 1).bit_length()
        side, crowd = min(PLANE, n), min(RAW, n)
        lines, groups = n // side, half // GROUP
        operands = table.T, mask.reshape(height // 128, 128), weight, bias.reshape(1, features)
        sem = pltpu.SemaphoreType.DMA
        loads = [
            pltpu.VMEM((half, height), F32),
            pltpu.VMEM((height // 128, 128), I32),
            pltpu.VMEM((1, width), F32),
        ]
        weights = [
            pltpu.VMEM((cols, width), F32),
            pltpu.VMEM((3 * cols + 16, width), BF16),
        ]
        if lines <= LINES:
            most = max(side, lines)
            block = pltpu.VMEM((most, half, height), F32)
            body = direct
            scratch = loads + [
                pltpu.VMEM((n, 1, 128), I32),
                pltpu.VMEM((n + 1, 1, 128), I32),
                block, block, block, block, block, block,
                pltpu.VMEM((sections, half, height), F32),
            ] + weights + [
                sem((4,)), sem((1,)), sem((3,)), sem((2,)),
                sem((groups,)), sem((groups,)), sem((groups,)), sem((groups,)),
                sem((1,)), pltpu.SemaphoreType.REGULAR,
            ]
        else:
            body = butterfly
            scratch = loads + [
                pltpu.VMEM((side, 1, 128), I32),
                pltpu.VMEM((n // side, 1, 128), I32),
                pltpu.VMEM((n + 1, 1, 128), I32),
                pltpu.VMEM((crowd, half, height), F32),
                pltpu.VMEM((levels, half, height), F32),
                pltpu.VMEM((levels, half, height), F32),
                pltpu.VMEM((sections, half, height), F32),
            ] + weights + [
                sem((levels + 1, CHUNKS)), sem((levels + 1, CHUNKS)),
                sem((crowd,)), sem((crowd,)),
                sem((side,)), sem((side,)),
                sem((n // side,)), sem((n // side,)),
                sem((4,)),
            ]
        return pl.pallas_call(
            functools.partial(body, n),
            name="filter_project",
            out_shape=jax.ShapeDtypeStruct((height, width), BF16),
            in_specs=[pl.BlockSpec(memory_space=pltpu.HBM)] * 4,
            out_specs=pl.BlockSpec(memory_space=pltpu.VMEM),
            scratch_shapes=scratch,
            compiler_params=pltpu.CompilerParams(
                collective_id=0, has_side_effects=True, vmem_limit_bytes=16 << 20
            ),
        )(*[pltpu.with_memory_space_constraint(x, pltpu.HBM) for x in operands])

    return jax.shard_map(
        step,
        mesh=mesh,
        in_specs=(P("rows", "section"), P("rows"), P(), P()),
        out_specs=P("rows", "section"),
        check_vma=False,
    )
```
